32 devices in a mesh: gy: 2 (over core), gx: 16 (over z, y, x).
Axes of the slice: x: 2, y: 2, z: 4, core: 2. Of those that a mesh axis runs over, the one named last changes fastest.
Arguments:
- basis_vectors: float32 [36, 64, 128, 256], P(None, 'gx', 'gy'), may hold values from -30 to 30, as said below
- reaction: float32 [64, 128, 256], P('gx', 'gy'), may hold values from 0.5 to 3
Outputs:
- new_vectors: float32 [4, 64, 128, 256], P(None, 'gx', 'gy')
- hessenberg: float32 [40, 4], replicated
The draws below stay inside these ranges and needn't reach their ends.
Inputs may be any that keep to these rules, and one draw needn't show every extreme that they name: `basis_vectors`: under the inner product the basis vectors are nearly orthonormal.
All inputs are finite; a program needn't handle non-finite values.
Results may differ from the reference program's by a relative error of at most 0.0003.
Values sent between devices are 32-bit elements; how exact they have to be, the bound alone decides.
A program may use at most 128 MiB of HBM per device.

```python
import math
import jax
import jax.numpy as jnp
from jax import lax

KEEP = 36
STEPS = 4
BASIS = 40
NX = 64
NY = 128
NZ = 256


WIND_SPEEDS = (0.9, 0.6, 0.4)


TILT_SHARE = 0.01


MIXING_SHARE = 0.003


RAMP_FACTOR = 3.0


def stencil_drawn(values, x_ext, y_ext, z_ext, reaction):
    summed = -reaction * values
    for position, extended in enumerate((x_ext, y_ext, z_ext)):
        count = values.shape[position]
        higher = lax.slice_in_dim(extended, 3, count + 3, axis=position)
        lower_one = lax.slice_in_dim(extended, 1, count + 1, axis=position)
        lower_two = lax.slice_in_dim(extended, 0, count, axis=position)
        wind_speed = WIND_SPEEDS[position]
        summed = summed + higher + lower_one - 2.0 * values - wind_speed * (3.0 * values - 4.0 * lower_one + lower_two) * 0.5
    return summed


def apply_operator_drawn(values, reaction):
    padded = jnp.pad(values, ((2, 1), (2, 1), (2, 1)))
    return stencil_drawn(values, padded[:, 2:-1, 2:-1], padded[2:-1, :, 2:-1], padded[2:-1, 2:-1, :], reaction)


def reaction_field(key):
    key_field = jax.random.fold_in(key, 7)
    shape = (NX, NY, NZ)
    return jax.random.uniform(key_field, shape, jnp.float32, 0.5, 3.0)


def draw_reaction(key, part):
    return reaction_field(key)


def rough_fields(key, count, plane_scale):
    shape = (count, NX, NY, NZ)
    values = jax.random.normal(key, shape, jnp.float32)
    return values * plane_scale


def draw_basis_vectors(key, part):
    key_list = jax.random.split(jax.random.fold_in(key, 11), 4)
    plane_index = jnp.arange(NX, dtype=jnp.float32).reshape(NX, 1, 1)
    plane_scale = jnp.exp(math.log(RAMP_FACTOR) * plane_index / float(NX - 1))
    plane_scale = plane_scale / jnp.sqrt(jnp.mean(plane_scale * plane_scale))
    seed_fields = rough_fields(key_list[0], 2, plane_scale)
    start_field = seed_fields[0] / jnp.sqrt(jnp.mean(seed_fields[0] * seed_fields[0]))
    image_field = apply_operator_drawn(start_field, reaction_field(key))
    tilted = image_field + TILT_SHARE * jnp.sqrt(jnp.mean(image_field * image_field)) * seed_fields[1]
    tilted = tilted - jnp.sum(tilted * start_field) / jnp.sum(start_field * start_field) * start_field
    tilted = tilted / jnp.sqrt(jnp.mean(tilted * tilted))
    row_fields = jnp.concatenate([start_field[None], tilted[None], rough_fields(key_list[1], KEEP - 2, plane_scale)], axis=0)
    gram_matrix = jnp.einsum('axyz,bxyz->ab', row_fields, row_fields, precision=lax.Precision.HIGHEST) / float(NX * NY * NZ)
    inverse = jnp.linalg.inv(jnp.linalg.cholesky(gram_matrix))
    moved_order = jnp.concatenate([jnp.arange(1, KEEP, dtype=jnp.int32), jnp.zeros((1,), jnp.int32)])
    shuffle = jnp.eye(KEEP, dtype=jnp.float32)[moved_order]
    mixing = jnp.eye(KEEP, dtype=jnp.float32) + MIXING_SHARE * jax.random.normal(key_list[2], (KEEP, KEEP), jnp.float32)
    matrix = jnp.dot(mixing, jnp.dot(shuffle, inverse, precision=lax.Precision.HIGHEST), precision=lax.Precision.HIGHEST)
    return jnp.einsum('ab,bxyz->axyz', matrix, row_fields, precision=lax.Precision.HIGHEST)


def setup_inputs(seed: int = 0) -> dict:
    splits = jax.random.split(jax.random.key(seed), 3)
    basis_vectors = draw_basis_vectors(jax.random.fold_in(splits[2], 71), 0)
    reaction = draw_reaction(jax.random.fold_in(splits[2], 71), 0)
    return {"basis_vectors": basis_vectors, "reaction": reaction}


WIND_SPEEDS = (0.9, 0.6, 0.4)
EPSILON = 1e-06

def stencil(values, x_ext, y_ext, z_ext, reaction):
    summed = -reaction * values
    for position, extended in enumerate((x_ext, y_ext, z_ext)):
        count = values.shape[position]
        higher = lax.slice_in_dim(extended, 3, count + 3, axis=position)
        lower_one = lax.slice_in_dim(extended, 1, count + 1, axis=position)
        lower_two = lax.slice_in_dim(extended, 0, count, axis=position)
        wind_speed = WIND_SPEEDS[position]
        summed = summed + higher + lower_one - 2.0 * values - wind_speed * (3.0 * values - 4.0 * lower_one + lower_two) * 0.5
    return summed

def apply_operator(values, reaction):
    padded = jnp.pad(values, ((2, 1), (2, 1), (2, 1)))
    return stencil(values, padded[:, 2:-1, 2:-1], padded[2:-1, :, 2:-1], padded[2:-1, 2:-1, :], reaction)

def project(basis_vectors, created, image):
    local = jnp.einsum('kxyz,xyz->k', basis_vectors, image, precision=lax.Precision.HIGHEST)
    extra = [jnp.sum(vector * image)[None] for vector in created]
    return jnp.concatenate([local] + extra)

def combine(basis_vectors, created, weights):
    keep_count = basis_vectors.shape[0]
    summed = jnp.einsum('k,kxyz->xyz', weights[:keep_count], basis_vectors, precision=lax.Precision.HIGHEST)
    for index, vector in enumerate(created):
        summed = summed + weights[keep_count + index] * vector
    return summed

def reference(basis_vectors, reaction):
    cell_count = float(NX * NY * NZ)
    created = []
    columns = []
    for section in range(STEPS):
        current = KEEP + section
        vector_now = basis_vectors[KEEP - 1] if section == 0 else created[-1]
        image = apply_operator(vector_now, reaction)
        first_terms = project(basis_vectors, created, image) / cell_count
        first_rest = image - combine(basis_vectors, created, first_terms)
        second_terms = project(basis_vectors, created, first_rest) / cell_count
        second_rest = first_rest - combine(basis_vectors, created, second_terms)
        length_now = jnp.sqrt(jnp.sum(second_rest * second_rest) / cell_count + EPSILON)
        columns.append(jnp.concatenate([first_terms + second_terms, length_now[None], jnp.zeros((BASIS - current - 1,), jnp.float32)]))
        created.append(second_rest / length_now)
    return (jnp.stack(created), jnp.stack(columns, axis=1))
```

```python
import functools

import jax
import jax.numpy as jnp
from jax import lax
from jax.experimental import pallas as pl
from jax.experimental.pallas import tpu as pltpu
from jax.sharding import PartitionSpec as P

STEPS = 4
WIND_SPEEDS = (0.9, 0.6, 0.4)
EPSILON = 1e-06
MESH = pl.DeviceIdType.MESH
CHUNK = 16


def roll(values, shift, axis):
    return pltpu.roll(values, shift, axis)


def fold_lanes(values):
    parts = [values[:, s : s + 128] for s in range(0, values.shape[1], 128)]
    return functools.reduce(lambda a, b: a + b, parts)


def tree(parts):
    while len(parts) > 1:
        parts = [
            parts[i] + parts[i + 1] if i + 1 < len(parts) else parts[i]
            for i in range(0, len(parts), 2)
        ]
    return parts[0]


def kernel(
    keep, planes, rows_y, n_gx, n_gy, g1,
    basis, reaction, w_out, h_out,
    vecs, padded, image, react, head, tail, squares, proj, slots1, slots2, slots, coef,
    load_sem, last_sem, react_sem,
    halo_send, halo_recv, send1, recv1, send2, recv2, sends, recvs, ready,
):
    width = basis.shape[2]
    rows = planes * rows_y
    padded_count = proj.shape[1]
    gx = lax.axis_index("gx")
    gy = lax.axis_index("gy")
    n1 = n_gy * g1
    n2 = n_gx // g1
    low = lax.rem(gx, g1)
    high = gx // g1
    me1 = gy * g1 + low
    me2 = high
    cells = float(rows * width * n_gx * n_gy)

    last_copies = [
        pltpu.make_async_copy(
            basis.at[keep - 1, p * rows_y : (p + 1) * rows_y],
            padded.at[0, p + 2, 8 : rows_y + 8],
            last_sem.at[p],
        )
        for p in range(planes)
    ]
    for copy in last_copies:
        copy.start()
    chunks = rows // CHUNK

    def load(c):
        at = pl.ds(pl.multiple_of(c * CHUNK, CHUNK), CHUNK)
        return pltpu.make_async_copy(basis.at[:, at], vecs.at[0:keep, at], load_sem.at[c])

    @pl.loop(0, chunks)
    def _(c):
        load(c).start()

    react_copy = pltpu.make_async_copy(reaction, react, react_sem)
    react_copy.start()

    has_xl, has_xh = gx > 0, gx < n_gx - 1
    has_yl, has_yh = gy > 0, gy < n_gy - 1

    def member1(d):
        p = lax.rem(me1 + d, n1)
        return p, {"gx": high * g1 + lax.rem(p, g1), "gy": p // g1}

    def member2(d):
        p = lax.rem(me2 + d, n2)
        return p, {"gx": p * g1 + low, "gy": gy}

    me = gx * n_gy + gy
    devices = n_gx * n_gy

    def member(d):
        p = lax.rem(me + d, devices)
        return {"gx": p // n_gy, "gy": lax.rem(p, n_gy)}

    barrier = pltpu.get_barrier_semaphore()
    for d in range(1, n1):
        pl.semaphore_signal(barrier, inc=1, device_id=member1(d)[1], device_id_type=MESH)
    for d in range(1, n2):
        pl.semaphore_signal(barrier, inc=1, device_id=member2(d)[1], device_id_type=MESH)
    sides = (
        (has_xh, {"gx": gx + 1, "gy": gy}),
        (has_xl, {"gx": gx - 1, "gy": gy}),
        (has_yh, {"gx": gx, "gy": gy + 1}),
        (has_yl, {"gx": gx, "gy": gy - 1}),
    )
    expected = n1 - 1 + n2 - 1
    for there, device in sides:
        @pl.when(there)
        def _(device=device):
            pl.semaphore_signal(barrier, inc=1, device_id=device, device_id_type=MESH)

        expected = expected + there.astype(jnp.int32)

    zero_plane = jnp.zeros((1, rows_y, width), jnp.float32)
    zero_rows = jnp.zeros((planes, 8, width), jnp.float32)
    for step in range(STEPS):
        @pl.when(jnp.logical_not(has_xl))
        def _(step=step):
            padded[step, 0:1, 8 : rows_y + 8] = zero_plane
            padded[step, 1:2, 8 : rows_y + 8] = zero_plane

        @pl.when(jnp.logical_not(has_xh))
        def _(step=step):
            padded[step, planes + 2 : planes + 3, 8 : rows_y + 8] = zero_plane

        @pl.when(jnp.logical_not(has_yl))
        def _(step=step):
            padded[step, 2 : planes + 2, 0:8] = zero_rows

        @pl.when(jnp.logical_not(has_yh))
        def _(step=step):
            padded[step, 2 : planes + 2, rows_y + 8 : rows_y + 16] = zero_rows

    head[...] = jnp.zeros(head.shape, jnp.float32)
    tail[...] = jnp.zeros(tail.shape, jnp.float32)
    squares[...] = jnp.zeros(squares.shape, jnp.float32)
    proj[...] = jnp.zeros(proj.shape, jnp.float32)
    pl.semaphore_wait(barrier, expected)
    for d in range(1, n2):
        pl.semaphore_signal(ready, inc=1, device_id=member2(d)[1], device_id_type=MESH)

    def halo_copies(step):
        own = pl.ds(2, planes)
        refs = (
            (padded.at[step, planes : planes + 2, 8 : rows_y + 8], padded.at[step, 0:2, 8 : rows_y + 8]),
            (padded.at[step, 2:3, 8 : rows_y + 8], padded.at[step, planes + 2 : planes + 3, 8 : rows_y + 8]),
            (padded.at[step, own, rows_y : rows_y + 8], padded.at[step, own, 0:8]),
            (padded.at[step, own, 8:16], padded.at[step, own, rows_y + 8 : rows_y + 16]),
        )
        return [
            pltpu.make_async_remote_copy(
                src_ref=src, dst_ref=dst,
                send_sem=halo_send.at[step, n], recv_sem=halo_recv.at[step, n],
                device_id=sides[n][1], device_id_type=MESH,
            )
            for n, (src, dst) in enumerate(refs)
        ]

    def start_halo(step, which):
        copies = halo_copies(step)
        for n in which:
            copy = copies[n]

            @pl.when(sides[n][0])
            def _(copy=copy):
                copy.start()

    def wait_halo(step, which):
        copies = halo_copies(step)
        arrives = (has_xl, has_xh, has_yl, has_yh)
        for n in which:
            copy = copies[n]

            @pl.when(arrives[n])
            def _(copy=copy):
                copy.wait_recv()

            @pl.when(sides[n][0])
            def _(copy=copy):
                copy.wait_send()

    stage1 = (slots1, me1, n1, member1, send1, recv1)
    stage2 = (slots2, me2, n2, member2, send2, recv2)

    def exchange(stage, begin):
        slots, me, count, member, send, recv = stage

        def copy_of(slot, d):
            return pltpu.make_async_remote_copy(
                src_ref=slots.at[slot], dst_ref=slots.at[slot],
                send_sem=send.at[d - 1], recv_sem=recv.at[slot],
                device_id=member(d)[1], device_id_type=MESH,
            )

        if begin:
            for d in range(1, count):
                copy_of(me, d).start()
            return None
        for d in range(1, count):
            copy_of(member(d)[0], d).wait_recv()
        for d in range(1, count):
            copy_of(me, d).wait_send()
        return tree([slots[slot] for slot in range(count)])

    def begin_sum(rnd, row):
        slots[rnd, me] = row
        for d in range(1, devices):
            pltpu.make_async_remote_copy(
                src_ref=slots.at[rnd, me], dst_ref=slots.at[rnd, me],
                send_sem=sends.at[rnd], recv_sem=recvs.at[rnd],
                device_id=member(d), device_id_type=MESH,
            ).start()

    def finish_sum(rnd):
        every = pltpu.make_async_remote_copy(
            src_ref=slots.at[rnd, 0 : devices - 1], dst_ref=slots.at[rnd, 0 : devices - 1],
            send_sem=sends.at[rnd], recv_sem=recvs.at[rnd],
            device_id=member(1), device_id_type=MESH,
        )
        every.wait_recv()
        every.wait_send()
        return tree([slots[rnd, slot] for slot in range(devices)]) / cells

    shape = (padded_count, 128)
    lane = lax.broadcasted_iota(jnp.int32, shape, 1)
    sub = lax.broadcasted_iota(jnp.int32, shape, 0)
    eye = lane == sub
    eye_high = lane == sub + 64
    lane8 = lax.broadcasted_iota(jnp.int32, (8, 128), 1)
    sub8 = lax.broadcasted_iota(jnp.int32, (8, 128), 0)

    def lane_sum(values):
        return jnp.broadcast_to(jnp.sum(values, axis=1, keepdims=True), values.shape)

    def to_column(row, where=eye):
        return lane_sum(jnp.where(where, jnp.broadcast_to(row, shape), 0.0))

    def to_row(column, where=eye):
        return jnp.sum(jnp.where(where, column, 0.0), axis=0, keepdims=True)

    def project(read, count, kind, spans, fresh):
        for first in range(0, count, 20):
            group = range(first, min(first + 20, count))

            def step(r, sums):
                at = pl.ds(pl.multiple_of(r * 8, 8), 8)
                other = read(at)
                return tuple(
                    acc + fold_lanes(vecs[i, at, :] * other) for i, acc in zip(group, sums)
                )

            if fresh:
                sums = (jnp.zeros((8, 128), jnp.float32),) * len(group)
            else:
                sums = tuple(proj[kind, i] for i in group)
            for start, stop in spans:
                sums = lax.fori_loop(start // 8, stop // 8, step, sums, unroll=4)
            for i, acc in zip(group, sums):
                proj[kind, i] = acc

    def projected(kind):
        return lane_sum(jnp.sum(proj[kind], axis=1))

    def stencil(step, part):
        tall = 16
        lanes = lax.broadcasted_iota(jnp.int32, (tall, width), 1)
        sx, sy, sz = WIND_SPEEDS
        centre = 6.0 + 1.5 * (sx + sy + sz)

        def piece(p, q):
            base = pl.multiple_of(q * tall, 8)
            at = pl.ds(pl.multiple_of(base + 8, 8), tall)
            block = padded[step, p + 2, pl.ds(base, tall + 16), :]
            here = block[8 : tall + 8]
            out_at = pl.ds(pl.multiple_of(p * rows_y + base, 8), tall)
            total = -(react[out_at, :] + centre) * here
            total = total + padded[step, p + 3, at, :]
            total = total + (1.0 + 2.0 * sx) * padded[step, p + 1, at, :]
            total = total - (0.5 * sx) * padded[step, p, at, :]
            total = total + roll(block, tall + 15, 0)[8 : tall + 8]
            total = total + (1.0 + 2.0 * sy) * roll(block, 1, 0)[8 : tall + 8]
            total = total - (0.5 * sy) * roll(block, 2, 0)[8 : tall + 8]
            total = total + jnp.where(lanes < width - 1, roll(here, width - 1, 1), 0.0)
            total = total + (1.0 + 2.0 * sz) * jnp.where(lanes >= 1, roll(here, 1, 1), 0.0)
            total = total - (0.5 * sz) * jnp.where(lanes >= 2, roll(here, 2, 1), 0.0)
            image[out_at, :] = total

        for p in part:
            @pl.loop(0, rows_y // tall, unroll=True)
            def _(q, p=p):
                piece(p, q)

    def combine(step, count, scale):
        tall = 32 if rows_y % 32 == 0 else 16
        scale_row = jnp.concatenate([scale] * (width // 128), axis=1)

        def plane(p):
            @pl.loop(0, rows_y // tall)
            def _(q):
                at = pl.ds(pl.multiple_of(p * rows_y + q * tall, 8), tall)
                total = image[at, :] * scale_row
                for i in range(count):
                    total = total - coef[i : i + 1, :] * vecs[i, at, :]
                vecs[keep + step, at, :] = total
                if step < STEPS - 1:
                    padded[step + 1, p + 2, pl.ds(pl.multiple_of(q * tall + 8, 8), tall), :] = total

        more = step < STEPS - 1
        done = []
        for part, side in (((planes - 2, planes - 1), 0), ((0,), 1), (range(planes), 2)):
            for p in part:
                if p not in done:
                    plane(p)
                    done.append(p)
            if more:
                start_halo(step + 1, (side,) if side < 2 else (2, 3))

    def split(values):
        scaled = values * 65537.0
        high = scaled - (scaled - values)
        return high, values - high

    def outer(a, b):
        return lax.dot_general(
            a, b, (((1,), (1,)), ((), ())), preferred_element_type=jnp.float32
        )

    cut = head.shape[1]
    late = keep * 8 - 128

    def gram_block(r):
        at = pl.ds(pl.multiple_of(r, 8), 8)
        values = vecs[0:keep, at, :].reshape(keep * 8, width)
        power = values * values
        squares[...] = squares[...] + power[:, :128] + power[:, 128:]
        high, low = split(values)
        left = jnp.concatenate([high[:cut] * 0.5, high[cut:]], axis=0)
        first = outer(left, high[:cut]) + outer(low, high[:cut])
        second = outer(low, high[late:])
        third = outer(high[cut:] * 0.5, high[late:])
        return first, second, third

    for copy in last_copies:
        copy.wait()
    start_halo(0, (0, 1, 2, 3))

    @pl.loop(0, chunks)
    def _(c):
        load(c).wait()
        found = [gram_block(c * CHUNK + s) for s in range(0, CHUNK, 8)]
        first, second, third = (functools.reduce(lambda a, b: a + b, f) for f in zip(*found))
        head[...] = head[...] + first
        tail[...] = tail[...] + second
        tail[cut:, :] = tail[cut:, :] + third

    def picked(values, start):
        row = lax.broadcasted_iota(jnp.int32, values.shape, 0)
        column = lax.broadcasted_iota(jnp.int32, values.shape, 1)
        use = (lax.rem(row, 8) == lax.rem(column, 8)) & (column + start >= (cut if start else 0))
        kept = jnp.where(use, values, 0.0)
        return jnp.sum(kept.reshape(keep, 8, values.shape[1]), axis=1)

    spread = jnp.concatenate([picked(head[...], 0), picked(tail[...], late)], axis=1)
    place = lax.broadcasted_iota(jnp.int32, (cut + 128, 128), 0)
    place = jnp.where(place < cut, place, place - cut + late) // 8
    choose = (place == lax.broadcasted_iota(jnp.int32, place.shape, 1)).astype(jnp.float32)
    exact = lax.Precision.HIGHEST
    half = jnp.dot(spread, choose, precision=exact, preferred_element_type=jnp.float32)
    turned = lax.dot_general(
        choose, spread, (((0,), (1,)), ((), ())), precision=exact,
        preferred_element_type=jnp.float32,
    )
    diagonal = jnp.sum(jnp.sum(squares[...].reshape(keep, 8, 128), axis=1), axis=1, keepdims=True)
    lane_k = lax.broadcasted_iota(jnp.int32, (keep, 128), 1)
    sub_k = lax.broadcasted_iota(jnp.int32, (keep, 128), 0)
    image[0:keep, 0:128] = half
    image[0:128, 128:256] = jnp.zeros((128, 128), jnp.float32)
    image[0:128, 128 : 128 + keep] = turned
    both = half + image[0:keep, 128:256]
    local_gram = jnp.where(lane_k == sub_k, diagonal, both)
    slots1[me1] = jnp.zeros(slots1.shape[1:], jnp.float32)
    slots1[me1, 0:keep] = local_gram
    react_copy.wait()
    exchange(stage1, True)

    everything = [(0, rows)]
    inner = range(2, planes - 1)
    edge = [p for p in range(planes) if p not in inner]
    inner_spans = [(p * rows_y, (p + 1) * rows_y) for p in inner]
    edge_spans = [(p * rows_y, (p + 1) * rows_y) for p in edge]

    def emit(step, scale):
        scale_row = jnp.concatenate([scale] * (width // 128), axis=1)

        @pl.loop(0, rows // 32)
        def _(q):
            at = pl.ds(pl.multiple_of(q * 32, 32), 32)
            w_out[step, at, :] = vecs[keep + step, at, :] * scale_row

    gram = None
    scales = jnp.ones(shape, jnp.float32)
    hess = jnp.zeros((8, 128), jnp.float32)
    b_row = jnp.zeros((1, 128), jnp.float32)
    scale = jnp.ones((1, 128), jnp.float32)
    for step in range(STEPS):
        count = keep + step
        last = count - 1
        if step > 0:
            project(lambda at: vecs[last, at, :], count, 1, everything, True)
            b_row = to_row(projected(1), eye_high)
        wait_halo(step, (2, 3))
        stencil(step, inner)
        project(lambda at: image[at, :], count, 0, inner_spans, True)
        if step > 1:
            emit(step - 2, scale)
        wait_halo(step, (0, 1))
        stencil(step, edge)
        project(lambda at: image[at, :], count, 0, edge_spans, False)
        row = to_row(projected(0)) + b_row
        if step == 0:
            pl.semaphore_wait(ready, n2 - 1)
        begin_sum(step, row)
        if step == 0:
            slots2[me2] = exchange(stage1, False)
            exchange(stage2, True)
            gram = exchange(stage2, False) / cells
            total = finish_sum(0)
        else:
            total = finish_sum(step)
            overlap = to_column(total, eye_high)
            norm = jnp.sqrt(overlap[last : last + 1] + EPSILON)
            scale = 1.0 / norm
            hess = jnp.where((sub8 == step - 1) & (lane8 == last), norm, hess)
            scales = jnp.where(sub == last, scale, scales)
            column = jnp.where(sub < count, overlap * scales * scale, 0.0)
            gram = jnp.where(sub == last, to_row(column), gram)
            gram = jnp.where(lane == last, column, gram)
        first = jnp.where(sub < count, to_column(total) * scales * scale, 0.0)
        weights = first + (first - lane_sum(gram * to_row(first)))
        weights = jnp.where(sub < count, weights, 0.0)
        scaled = weights * scales
        coef[...] = jnp.concatenate([scaled] * (width // 128), axis=1)
        combine(step, count, scale)
        hess = jnp.where(sub8 == step, to_row(weights), hess)

    last = keep + STEPS - 1

    def square(r, acc):
        values = vecs[last, pl.ds(pl.multiple_of(r * 8, 8), 8), :]
        return acc + fold_lanes(values * values)

    acc = lax.fori_loop(0, rows // 8, square, jnp.zeros((8, 128), jnp.float32), unroll=4)
    begin_sum(STEPS, lane_sum(jnp.sum(acc, axis=0, keepdims=True)))
    emit(STEPS - 2, scale)
    total = finish_sum(STEPS)
    norm = jnp.sqrt(total + EPSILON)
    hess = jnp.where((sub8 == STEPS - 1) & (lane8 == last), norm, hess)
    h_out[...] = hess
    emit(STEPS - 1, 1.0 / norm)


def group_of(count):
    for size in (4, 2):
        if count % size == 0:
            return size
    return 1


def body(basis_vectors, reaction):
    keep, planes, rows_y, width = basis_vectors.shape
    n_gx, n_gy = lax.axis_size("gx"), lax.axis_size("gy")
    g1 = group_of(n_gx)
    n1, n2 = g1 * n_gy, n_gx // g1
    size = keep + STEPS
    padded_count = -(-size // 8) * 8
    rows = planes * rows_y
    rounds = STEPS + 1
    f32 = jnp.float32
    dma = pltpu.SemaphoreType.DMA
    w, h = pl.pallas_call(
        functools.partial(kernel, keep, planes, rows_y, n_gx, n_gy, g1),
        out_shape=(
            jax.ShapeDtypeStruct((STEPS, rows, width), f32),
            jax.ShapeDtypeStruct((8, 128), f32),
        ),
        in_specs=[pl.BlockSpec(memory_space=pltpu.HBM)] * 2,
        out_specs=(pl.BlockSpec(memory_space=pltpu.VMEM),) * 2,
        scratch_shapes=[
            pltpu.VMEM((size, rows, width), f32),
            pltpu.VMEM((STEPS, planes + 3, rows_y + 16, width), f32),
            pltpu.VMEM((rows, width), f32),
            pltpu.VMEM((rows, width), f32),
            pltpu.VMEM((keep * 8, 256), f32),
            pltpu.VMEM((keep * 8, 128), f32),
            pltpu.VMEM((keep * 8, 128), f32),
            pltpu.VMEM((2, padded_count, 8, 128), f32),
            pltpu.VMEM((n1, padded_count, 128), f32),
            pltpu.VMEM((n2, padded_count, 128), f32),
            pltpu.VMEM((rounds, n_gx * n_gy, 1, 128), f32),
            pltpu.VMEM((padded_count, width), f32),
            dma((rows // CHUNK,)),
            dma((planes,)),
            dma,
            dma((STEPS, 4)),
            dma((STEPS, 4)),
            dma((n1,)),
            dma((n1,)),
            dma((n2,)),
            dma((n2,)),
            dma((rounds,)),
            dma((rounds,)),
            pltpu.SemaphoreType.REGULAR,
        ],
        compiler_params=pltpu.CompilerParams(
            collective_id=0, has_side_effects=True, vmem_limit_bytes=48 * 1024 * 1024
        ),
    )(basis_vectors.reshape(keep, rows, width), reaction.reshape(rows, width))
    return w.reshape(STEPS, planes, rows_y, width), h[:STEPS, :size].T


def solution(mesh):
    in_specs = (P(None, "gx", "gy", None), P("gx", "gy", None))
    out_specs = (P(None, "gx", "gy", None), P())
    return jax.shard_map(body, mesh=mesh, in_specs=in_specs, out_specs=out_specs, check_vma=False)
```

```python
import functools

import jax
import jax.numpy as jnp
from jax import lax
from jax.experimental import pallas as pl
from jax.experimental.pallas import tpu as pltpu
from jax.sharding import PartitionSpec as P

STEPS = 4
WIND_SPEEDS = (0.9, 0.6, 0.4)
EPSILON = 1e-06
MESH = pl.DeviceIdType.MESH
CHUNK = 32


def roll(values, shift, axis):
    return pltpu.roll(values, shift, axis)


def fold_lanes(values):
    parts = [values[:, s : s + 128] for s in range(0, values.shape[1], 128)]
    return functools.reduce(lambda a, b: a + b, parts)


def tree(parts):
    while len(parts) > 1:
        parts = [
            parts[i] + parts[i + 1] if i + 1 < len(parts) else parts[i]
            for i in range(0, len(parts), 2)
        ]
    return parts[0]


def kernel(
    keep, planes, rows_y, n_gx, n_gy, g1,
    basis, reaction, w_out, h_out,
    vecs, padded, image, react, head, tail, squares, pack, proj, slots1, slots2, slots, coef,
    load_sem, last_sem, react_sem,
    halo_send, halo_recv, send1, recv1, send2, recv2, sends, recvs, ready,
):
    width = basis.shape[2]
    rows = planes * rows_y
    padded_count = proj.shape[1]
    gx = lax.axis_index("gx")
    gy = lax.axis_index("gy")
    n1 = n_gy * g1
    n2 = n_gx // g1
    low = lax.rem(gx, g1)
    high = gx // g1
    me1 = gy * g1 + low
    me2 = high
    cells = float(rows * width * n_gx * n_gy)

    last_copies = [
        pltpu.make_async_copy(
            basis.at[keep - 1, p * rows_y : (p + 1) * rows_y],
            padded.at[0, p + 2, 8 : rows_y + 8],
            last_sem.at[p],
        )
        for p in range(planes)
    ]
    for copy in last_copies:
        copy.start()
    chunks = rows // CHUNK

    def load(c):
        at = pl.ds(pl.multiple_of(c * CHUNK, CHUNK), CHUNK)
        return pltpu.make_async_copy(basis.at[:, at], vecs.at[0:keep, at], load_sem.at[c])

    @pl.loop(0, chunks)
    def _(c):
        load(c).start()

    react_copy = pltpu.make_async_copy(reaction, react, react_sem)
    react_copy.start()

    has_xl, has_xh = gx > 0, gx < n_gx - 1
    has_yl, has_yh = gy > 0, gy < n_gy - 1

    def member1(d):
        p = lax.rem(me1 + d, n1)
        return p, {"gx": high * g1 + lax.rem(p, g1), "gy": p // g1}

    def member2(d):
        p = lax.rem(me2 + d, n2)
        return p, {"gx": p * g1 + low, "gy": gy}

    me = gx * n_gy + gy
    devices = n_gx * n_gy

    def member(d):
        p = lax.rem(me + d, devices)
        return {"gx": p // n_gy, "gy": lax.rem(p, n_gy)}

    barrier = pltpu.get_barrier_semaphore()
    for d in range(1, n1):
        pl.semaphore_signal(barrier, inc=1, device_id=member1(d)[1], device_id_type=MESH)
    for d in range(1, n2):
        pl.semaphore_signal(barrier, inc=1, device_id=member2(d)[1], device_id_type=MESH)
    sides = (
        (has_xh, {"gx": gx + 1, "gy": gy}),
        (has_xl, {"gx": gx - 1, "gy": gy}),
        (has_yh, {"gx": gx, "gy": gy + 1}),
        (has_yl, {"gx": gx, "gy": gy - 1}),
    )
    even = lax.rem(gx, 2) == 0
    odd = jnp.logical_not(even)
    expected = n1 - 1 + n2 - 1
    for there, device in sides:
        @pl.when(there)
        def _(device=device):
            pl.semaphore_signal(barrier, inc=1, device_id=device, device_id_type=MESH)

        expected = expected + there.astype(jnp.int32)

    zero_plane = jnp.zeros((1, rows_y, width), jnp.float32)
    zero_rows = jnp.zeros((planes, 8, width), jnp.float32)
    for step in range(STEPS):
        @pl.when(jnp.logical_not(has_xl))
        def _(step=step):
            padded[step, 0:1, 8 : rows_y + 8] = zero_plane
            padded[step, 1:2, 8 : rows_y + 8] = zero_plane

        @pl.when(jnp.logical_not(has_xh))
        def _(step=step):
            padded[step, planes + 2 : planes + 3, 8 : rows_y + 8] = zero_plane

        @pl.when(jnp.logical_not(has_yl))
        def _(step=step):
            padded[step, 2 : planes + 2, 0:8] = zero_rows

        @pl.when(jnp.logical_not(has_yh))
        def _(step=step):
            padded[step, 2 : planes + 2, rows_y + 8 : rows_y + 16] = zero_rows

    head[...] = jnp.zeros(head.shape, jnp.float32)
    tail[...] = jnp.zeros(tail.shape, jnp.float32)
    squares[...] = jnp.zeros(squares.shape, jnp.float32)
    proj[...] = jnp.zeros(proj.shape, jnp.float32)
    def halo_copies(step):
        own = pl.ds(2, planes)
        inside = slice(8, rows_y + 8)
        refs = (
            (0, padded.at[step, planes + 1, inside], padded.at[step, 1, inside]),
            (0, padded.at[step, planes, inside], padded.at[step, 0, inside]),
            (1, padded.at[step, 2, inside], padded.at[step, planes + 2, inside]),
            (2, padded.at[step, own, rows_y : rows_y + 8], padded.at[step, own, 0:8]),
            (3, padded.at[step, own, 8:16], padded.at[step, own, rows_y + 8 : rows_y + 16]),
        )
        return [
            (
                sides[side][0],
                (has_xl, has_xh, has_yl, has_yh)[side],
                pltpu.make_async_remote_copy(
                    src_ref=src, dst_ref=dst,
                    send_sem=halo_send.at[step, n], recv_sem=halo_recv.at[step, n],
                    device_id=sides[side][1], device_id_type=MESH,
                ),
            )
            for n, (side, src, dst) in enumerate(refs)
        ]

    def start_halo(step, which, where=None):
        copies = halo_copies(step)
        for n in which:
            there, _, copy = copies[n]

            @pl.when(there if where is None else there & where)
            def _(copy=copy):
                copy.start()

    def wait_halo(step, which, where=None):
        copies = halo_copies(step)
        for n in which:
            _, arrives, copy = copies[n]

            @pl.when(arrives if where is None else arrives & where)
            def _(copy=copy):
                copy.wait_recv()

    def drain_halo(step):
        for there, _, copy in halo_copies(step):
            @pl.when(there)
            def _(copy=copy):
                copy.wait_send()

    stage1 = (slots1, me1, n1, member1, send1, recv1)
    stage2 = (slots2, me2, n2, member2, send2, recv2)

    def exchange(stage, begin):
        slots, me, count, member, send, recv = stage

        def copy_of(slot, d):
            return pltpu.make_async_remote_copy(
                src_ref=slots.at[slot], dst_ref=slots.at[slot],
                send_sem=send.at[d - 1], recv_sem=recv.at[slot],
                device_id=member(d)[1], device_id_type=MESH,
            )

        if begin:
            for d in range(1, count):
                copy_of(me, d).start()
            return None
        for d in range(1, count):
            copy_of(member(d)[0], d).wait_recv()
        for d in range(1, count):
            copy_of(me, d).wait_send()
        return tree([slots[slot] for slot in range(count)])

    def begin_sum(rnd, row):
        slots[rnd, me] = row
        for d in range(1, devices):
            pltpu.make_async_remote_copy(
                src_ref=slots.at[rnd, me], dst_ref=slots.at[rnd, me],
                send_sem=sends.at[rnd], recv_sem=recvs.at[rnd],
                device_id=member(d), device_id_type=MESH,
            ).start()

    def every(rnd):
        return pltpu.make_async_remote_copy(
            src_ref=slots.at[rnd, 0 : devices - 1], dst_ref=slots.at[rnd, 0 : devices - 1],
            send_sem=sends.at[rnd], recv_sem=recvs.at[rnd],
            device_id=member(1), device_id_type=MESH,
        )

    def finish_sum(rnd):
        every(rnd).wait_recv()
        return tree([slots[rnd, slot] for slot in range(devices)]) / cells

    shape = (padded_count, 128)
    lane = lax.broadcasted_iota(jnp.int32, shape, 1)
    sub = lax.broadcasted_iota(jnp.int32, shape, 0)
    eye = lane == sub
    eye_high = lane == sub + 64
    lane8 = lax.broadcasted_iota(jnp.int32, (8, 128), 1)
    sub8 = lax.broadcasted_iota(jnp.int32, (8, 128), 0)

    def lane_sum(values):
        return jnp.broadcast_to(jnp.sum(values, axis=1, keepdims=True), values.shape)

    def to_column(row, where=eye):
        return lane_sum(jnp.where(where, jnp.broadcast_to(row, shape), 0.0))

    def to_row(column, where=eye):
        return jnp.sum(jnp.where(where, column, 0.0), axis=0, keepdims=True)

    def project(read, count, kind, spans, fresh):
        for first in range(0, count, 20):
            group = range(first, min(first + 20, count))

            def step(r, sums):
                at = pl.ds(pl.multiple_of(r * 8, 8), 8)
                other = read(at)
                return tuple(
                    acc + fold_lanes(vecs[i, at, :] * other) for i, acc in zip(group, sums)
                )

            if fresh:
                sums = (jnp.zeros((8, 128), jnp.float32),) * len(group)
            else:
                sums = tuple(proj[kind, i] for i in group)
            for start, length in spans:
                base = start // 8
                sums = lax.fori_loop(0, length // 8, lambda r, s: step(base + r, s), sums, unroll=4)
            for i, acc in zip(group, sums):
                proj[kind, i] = acc

    def projected(kind):
        return lane_sum(jnp.sum(proj[kind], axis=1))

    def stencil(step, part):
        tall = 16
        lanes = lax.broadcasted_iota(jnp.int32, (tall, width), 1)
        sx, sy, sz = WIND_SPEEDS
        centre = 6.0 + 1.5 * (sx + sy + sz)

        def piece(p, q):
            base = pl.multiple_of(q * tall, 8)
            at = pl.ds(pl.multiple_of(base + 8, 8), tall)
            block = padded[step, p + 2, pl.ds(base, tall + 16), :]
            here = block[8 : tall + 8]
            out_at = pl.ds(pl.multiple_of(p * rows_y + base, 8), tall)
            total = -(react[out_at, :] + centre) * here
            total = total + padded[step, p + 3, at, :]
            total = total + (1.0 + 2.0 * sx) * padded[step, p + 1, at, :]
            total = total - (0.5 * sx) * padded[step, p, at, :]
            total = total + roll(block, tall + 15, 0)[8 : tall + 8]
            total = total + (1.0 + 2.0 * sy) * roll(block, 1, 0)[8 : tall + 8]
            total = total - (0.5 * sy) * roll(block, 2, 0)[8 : tall + 8]
            total = total + jnp.where(lanes < width - 1, roll(here, width - 1, 1), 0.0)
            total = total + (1.0 + 2.0 * sz) * jnp.where(lanes >= 1, roll(here, 1, 1), 0.0)
            total = total - (0.5 * sz) * jnp.where(lanes >= 2, roll(here, 2, 1), 0.0)
            image[out_at, :] = total

        for p in part:
            @pl.loop(0, rows_y // tall, unroll=True)
            def _(q, p=p):
                piece(p, q)

    def combine(step, count, scale):
        tall = next(t for t in (64, 32, 16, 8) if rows_y % t == 0)
        scale_row = jnp.concatenate([scale] * (width // 128), axis=1)
        more = step < STEPS - 1

        def plane(p):
            @pl.loop(0, rows_y // tall)
            def _(q):
                at = pl.ds(pl.multiple_of(p * rows_y + q * tall, 8), tall)
                total = image[at, :] * scale_row
                for i in range(count):
                    total = total - coef[i : i + 1, :] * vecs[i, at, :]
                vecs[keep + step, at, :] = total
                if more:
                    padded[step + 1, p + 2, pl.ds(pl.multiple_of(q * tall + 8, 8), tall), :] = total

        for p_even, p_odd, n_even, n_odd in (
            (0, planes - 1, 2, 0),
            (planes - 1, planes - 2, 0, 1),
            (planes - 2, 0, 1, 2),
        ):
            plane(jnp.where(even, p_even, p_odd))
            if more:
                start_halo(step + 1, (n_even,), even)
                start_halo(step + 1, (n_odd,), odd)
        for p in range(1, planes - 2):
            plane(p)
        if more:
            start_halo(step + 1, (3, 4))

    def outer(a, b):
        return lax.dot_general(
            a, b, (((1,), (1,)), ((), ())), preferred_element_type=jnp.float32
        )

    cut = head.shape[1]
    late = keep * 8 - 128

    def gram_block(r):
        at = pl.ds(pl.multiple_of(r, 8), 8)
        values = vecs[0:keep, at, :].reshape(keep * 8, width)
        power = values * values
        squares[...] = squares[...] + power[:, :128] + power[:, 128:]
        high = values.astype(jnp.bfloat16)
        low = (values - high.astype(jnp.float32)).astype(jnp.bfloat16)
        left = jnp.concatenate([high[:cut] * 0.5, high[cut:]], axis=0)
        first = outer(left, high[:cut]) + outer(low, high[:cut])
        second = outer(low, high[late:])
        third = outer(high[cut:] * 0.5, high[late:])
        return first, second, third

    @pl.loop(0, chunks)
    def _(c):
        @pl.when(c == 1)
        def _():
            pl.semaphore_wait(barrier, expected)
            for d in range(1, n2):
                pl.semaphore_signal(ready, inc=1, device_id=member2(d)[1], device_id_type=MESH)
            for copy in last_copies:
                copy.wait()
            start_halo(0, (2, 0, 1), even)
            start_halo(0, (0, 1, 2), odd)
            start_halo(0, (3, 4))

        load(c).wait()
        found = [gram_block(c * CHUNK + s) for s in range(0, CHUNK, 8)]
        first, second, third = (functools.reduce(lambda a, b: a + b, f) for f in zip(*found))
        head[...] = head[...] + first
        tail[...] = tail[...] + second
        tail[cut:, :] = tail[cut:, :] + third

    def picked(values, start):
        row = lax.broadcasted_iota(jnp.int32, values.shape, 0)
        column = lax.broadcasted_iota(jnp.int32, values.shape, 1)
        use = (lax.rem(row, 8) == lax.rem(column, 8)) & (column + start >= (cut if start else 0))
        kept = jnp.where(use, values, 0.0)
        return jnp.sum(kept.reshape(keep, 8, values.shape[1]), axis=1)

    spread = jnp.concatenate([picked(head[...], 0), picked(tail[...], late)], axis=1)
    place = lax.broadcasted_iota(jnp.int32, (cut + 128, 128), 0)
    place = jnp.where(place < cut, place, place - cut + late) // 8
    choose = jnp.where(place == lax.broadcasted_iota(jnp.int32, place.shape, 1), 1.0, 0.0)
    choose = choose.astype(jnp.bfloat16)
    half = jnp.zeros((keep, 128), jnp.float32)
    for _ in range(3):
        term = spread.astype(jnp.bfloat16)
        spread = spread - term.astype(jnp.float32)
        half = half + jnp.dot(term, choose, preferred_element_type=jnp.float32)
    diagonal = jnp.sum(jnp.sum(squares[...].reshape(keep, 8, 128), axis=1), axis=1, keepdims=True)
    lane_k = lax.broadcasted_iota(jnp.int32, (keep, 128), 1)
    sub_k = lax.broadcasted_iota(jnp.int32, (keep, 128), 0)
    image[0:128, 0:128] = jnp.zeros((128, 128), jnp.float32)
    image[0:keep, 0:128] = half
    turned = jnp.transpose(image[0:128, 0:128])
    pack[...] = jnp.zeros(pack.shape, jnp.float32)
    pack[0:keep] = jnp.where(lane_k == sub_k, diagonal, half + turned[0:keep])
    band = slots1.shape[1]
    folded = jnp.zeros((band, 128), jnp.float32)
    bands = [(g, g * band, min(g * band + band, padded_count)) for g in range(-(-padded_count // band))]
    for g, start, stop in bands:
        part = pack[start:stop]
        if stop - start < band:
            part = jnp.concatenate([part, jnp.zeros((band - stop + start, 128), jnp.float32)], axis=0)
        folded = folded + (roll(part, g * padded_count, 1) if g else part)
    slots1[me1] = folded

    def unfold(values):
        parts = [
            (roll(values, 128 - g * padded_count, 1) if g else values)[0 : stop - start]
            for g, start, stop in bands
        ]
        return jnp.where(lane < padded_count, jnp.concatenate(parts, axis=0), 0.0)

    react_copy.wait()
    exchange(stage1, True)

    everything = [(0, rows)]

    def span(p, n=1):
        return [(p * rows_y, n * rows_y)]

    def edge(step, p):
        stencil(step, [p])
        project(lambda at: image[at, :], keep + step, 0, span(p), False)

    def emit(step, scale):
        scale_row = jnp.concatenate([scale] * (width // 128), axis=1)

        @pl.loop(0, rows // 32)
        def _(q):
            at = pl.ds(pl.multiple_of(q * 32, 32), 32)
            w_out[step, at, :] = vecs[keep + step, at, :] * scale_row

    gram = None
    scales = jnp.ones(shape, jnp.float32)
    hess = jnp.zeros((8, 128), jnp.float32)
    b_row = jnp.zeros((1, 128), jnp.float32)
    scale = jnp.ones((1, 128), jnp.float32)
    for step in range(STEPS):
        count = keep + step
        last = count - 1
        if step > 0:
            project(lambda at: vecs[last, at, :], count, 1, everything, True)
            b_row = to_row(projected(1), eye_high)
        wait_halo(step, (3, 4))
        stencil(step, range(2, planes - 1))
        project(lambda at: image[at, :], count, 0, span(2, planes - 3), True)
        if step > 1:
            emit(step - 2, scale)
        wait_halo(step, (0,))
        edge(step, 1)
        for p_even, p_odd, n_even, n_odd in ((0, planes - 1, 1, 2), (planes - 1, 0, 2, 1)):
            wait_halo(step, (n_even,), even)
            wait_halo(step, (n_odd,), odd)
            edge(step, jnp.where(even, p_even, p_odd))
        row = to_row(projected(0)) + b_row
        if step == 0:
            pl.semaphore_wait(ready, n2 - 1)
        begin_sum(step, row)
        if step == 0:
            slots2[me2] = exchange(stage1, False)
            exchange(stage2, True)
            gram = unfold(exchange(stage2, False) / cells)
            total = finish_sum(0)
        else:
            total = finish_sum(step)
            overlap = to_column(total, eye_high)
            norm = jnp.sqrt(overlap[last : last + 1] + EPSILON)
            scale = 1.0 / norm
            hess = jnp.where((sub8 == step - 1) & (lane8 == last), norm, hess)
            scales = jnp.where(sub == last, scale, scales)
            column = jnp.where(sub < count, overlap * scales * scale, 0.0)
            gram = jnp.where(sub == last, to_row(column), gram)
            gram = jnp.where(lane == last, column, gram)
        first = jnp.where(sub < count, to_column(total) * scales * scale, 0.0)
        weights = first + (first - lane_sum(gram * to_row(first)))
        weights = jnp.where(sub < count, weights, 0.0)
        scaled = weights * scales
        coef[...] = jnp.concatenate([scaled] * (width // 128), axis=1)
        combine(step, count, scale)
        hess = jnp.where(sub8 == step, to_row(weights), hess)

    last = keep + STEPS - 1

    def square(r, acc):
        values = vecs[last, pl.ds(pl.multiple_of(r * 8, 8), 8), :]
        return acc + fold_lanes(values * values)

    acc = lax.fori_loop(0, rows // 8, square, jnp.zeros((8, 128), jnp.float32), unroll=4)
    begin_sum(STEPS, lane_sum(jnp.sum(acc, axis=0, keepdims=True)))
    emit(STEPS - 2, scale)
    total = finish_sum(STEPS)
    norm = jnp.sqrt(total + EPSILON)
    hess = jnp.where((sub8 == STEPS - 1) & (lane8 == last), norm, hess)
    h_out[...] = hess
    emit(STEPS - 1, 1.0 / norm)
    for step in range(STEPS):
        drain_halo(step)
    for rnd in range(STEPS + 1):
        every(rnd).wait_send()


def group_of(count):
    for size in (4, 2):
        if count % size == 0:
            return size
    return 1


def body(basis_vectors, reaction):
    keep, planes, rows_y, width = basis_vectors.shape
    n_gx, n_gy = lax.axis_size("gx"), lax.axis_size("gy")
    g1 = group_of(n_gx)
    n1, n2 = g1 * n_gy, n_gx // g1
    size = keep + STEPS
    padded_count = -(-size // 8) * 8
    rows = planes * rows_y
    rounds = STEPS + 1
    band = -(-padded_count // (128 // padded_count) // 8) * 8
    f32 = jnp.float32
    dma = pltpu.SemaphoreType.DMA
    held = [
        pltpu.with_memory_space_constraint(x, pltpu.HBM)
        for x in (basis_vectors.reshape(keep, rows, width), reaction.reshape(rows, width))
    ]
    w, h = pl.pallas_call(
        functools.partial(kernel, keep, planes, rows_y, n_gx, n_gy, g1),
        out_shape=(
            jax.ShapeDtypeStruct((STEPS, rows, width), f32),
            jax.ShapeDtypeStruct((8, 128), f32),
        ),
        in_specs=[pl.BlockSpec(memory_space=pltpu.HBM)] * 2,
        out_specs=(pl.BlockSpec(memory_space=pltpu.VMEM),) * 2,
        scratch_shapes=[
            pltpu.VMEM((size, rows, width), f32),
            pltpu.VMEM((STEPS, planes + 3, rows_y + 16, width), f32),
            pltpu.VMEM((rows, width), f32),
            pltpu.VMEM((rows, width), f32),
            pltpu.VMEM((keep * 8, 256), f32),
            pltpu.VMEM((keep * 8, 128), f32),
            pltpu.VMEM((keep * 8, 128), f32),
            pltpu.VMEM((padded_count, 128), f32),
            pltpu.VMEM((2, padded_count, 8, 128), f32),
            pltpu.VMEM((n1, band, 128), f32),
            pltpu.VMEM((n2, band, 128), f32),
            pltpu.VMEM((rounds, n_gx * n_gy, 1, 128), f32),
            pltpu.VMEM((padded_count, width), f32),
            dma((rows // CHUNK,)),
            dma((planes,)),
            dma,
            dma((STEPS, 5)),
            dma((STEPS, 5)),
            dma((n1,)),
            dma((n1,)),
            dma((n2,)),
            dma((n2,)),
            dma((rounds,)),
            dma((rounds,)),
            pltpu.SemaphoreType.REGULAR,
        ],
        compiler_params=pltpu.CompilerParams(
            collective_id=0, has_side_effects=True, vmem_limit_bytes=48 * 1024 * 1024
        ),
    )(*held)
    return w.reshape(STEPS, planes, rows_y, width), h[:STEPS, :size].T


def solution(mesh):
    in_specs = (P(None, "gx", "gy", None), P("gx", "gy", None))
    out_specs = (P(None, "gx", "gy", None), P())
    return jax.shard_map(body, mesh=mesh, in_specs=in_specs, out_specs=out_specs, check_vma=False)
```

```python
import functools

import jax
import jax.numpy as jnp
from jax import lax
from jax.experimental import pallas as pl
from jax.experimental.pallas import tpu as pltpu
from jax.sharding import PartitionSpec as P

STEPS = 4
WIND_SPEEDS = (0.9, 0.6, 0.4)
EPSILON = 1e-06
MESH = pl.DeviceIdType.MESH
CHUNK = 32


def roll(values, shift, axis):
    return pltpu.roll(values, shift, axis)


def fold_lanes(values):
    parts = [values[:, s : s + 128] for s in range(0, values.shape[1], 128)]
    return functools.reduce(lambda a, b: a + b, parts)


def tree(parts):
    while len(parts) > 1:
        parts = [
            parts[i] + parts[i + 1] if i + 1 < len(parts) else parts[i]
            for i in range(0, len(parts), 2)
        ]
    return parts[0]


def two_sum(a, b):
    total = a + b
    other = total - a
    return total, (a - (total - other)) + (b - other)


def halves(a):
    scaled = a * 4097.0
    high = scaled - (scaled - a)
    return high, a - high


def two_product(a, b):
    product = a * b
    ah, al = halves(a)
    bh, bl = halves(b)
    return product, ((ah * bh - product) + ah * bl + al * bh) + al * bl


def exact_tree(parts):
    def add(a, b):
        total, rest = two_sum(a[0], b[0])
        return total, (a[1] + b[1]) + rest

    pairs = [(part, jnp.zeros_like(part)) for part in parts]
    while len(pairs) > 1:
        pairs = [
            add(pairs[i], pairs[i + 1]) if i + 1 < len(pairs) else pairs[i]
            for i in range(0, len(pairs), 2)
        ]
    return pairs[0]


def kernel(
    keep, planes, rows_y, n_gx, n_gy, g1,
    basis, reaction, w_out, h_out,
    vecs, padded, image, react, head, tail, squares, pack, proj, slots1, slots2, slots, coef,
    load_sem, last_sem, react_sem,
    halo_send, halo_recv, send1, recv1, send2, recv2, sends, recvs, ready,
):
    width = basis.shape[2]
    rows = planes * rows_y
    padded_count = proj.shape[1]
    gx = lax.axis_index("gx")
    gy = lax.axis_index("gy")
    n1 = n_gy * g1
    n2 = n_gx // g1
    low = lax.rem(gx, g1)
    high = gx // g1
    me1 = gy * g1 + low
    me2 = high
    cells = float(rows * width * n_gx * n_gy)

    last_copies = [
        pltpu.make_async_copy(
            basis.at[keep - 1, p * rows_y : (p + 1) * rows_y],
            padded.at[0, p + 2, 8 : rows_y + 8],
            last_sem.at[p],
        )
        for p in range(planes)
    ]
    for copy in last_copies:
        copy.start()
    chunks = rows // CHUNK

    def load(c):
        at = pl.ds(pl.multiple_of(c * CHUNK, CHUNK), CHUNK)
        return pltpu.make_async_copy(basis.at[:, at], vecs.at[0:keep, at], load_sem.at[c])

    @pl.loop(0, chunks)
    def _(c):
        load(c).start()

    react_copy = pltpu.make_async_copy(reaction, react, react_sem)
    react_copy.start()

    has_xl, has_xh = gx > 0, gx < n_gx - 1
    has_yl, has_yh = gy > 0, gy < n_gy - 1

    def member1(d):
        p = lax.rem(me1 + d, n1)
        return p, {"gx": high * g1 + lax.rem(p, g1), "gy": p // g1}

    def member2(d):
        p = lax.rem(me2 + d, n2)
        return p, {"gx": p * g1 + low, "gy": gy}

    me = gx * n_gy + gy
    devices = n_gx * n_gy

    def member(d):
        p = lax.rem(me + d, devices)
        return {"gx": p // n_gy, "gy": lax.rem(p, n_gy)}

    barrier = pltpu.get_barrier_semaphore()
    for d in range(1, n1):
        pl.semaphore_signal(barrier, inc=1, device_id=member1(d)[1], device_id_type=MESH)
    for d in range(1, n2):
        pl.semaphore_signal(barrier, inc=1, device_id=member2(d)[1], device_id_type=MESH)
    sides = (
        (has_xh, {"gx": gx + 1, "gy": gy}),
        (has_xl, {"gx": gx - 1, "gy": gy}),
        (has_yh, {"gx": gx, "gy": gy + 1}),
        (has_yl, {"gx": gx, "gy": gy - 1}),
    )
    even = lax.rem(gx, 2) == 0
    odd = jnp.logical_not(even)
    expected = n1 - 1 + n2 - 1
    for there, device in sides:
        @pl.when(there)
        def _(device=device):
            pl.semaphore_signal(barrier, inc=1, device_id=device, device_id_type=MESH)

        expected = expected + there.astype(jnp.int32)

    zero_plane = jnp.zeros((1, rows_y, width), jnp.float32)
    zero_rows = jnp.zeros((planes, 8, width), jnp.float32)
    for step in range(STEPS):
        @pl.when(jnp.logical_not(has_xl))
        def _(step=step):
            padded[step, 0:1, 8 : rows_y + 8] = zero_plane
            padded[step, 1:2, 8 : rows_y + 8] = zero_plane

        @pl.when(jnp.logical_not(has_xh))
        def _(step=step):
            padded[step, planes + 2 : planes + 3, 8 : rows_y + 8] = zero_plane

        @pl.when(jnp.logical_not(has_yl))
        def _(step=step):
            padded[step, 2 : planes + 2, 0:8] = zero_rows

        @pl.when(jnp.logical_not(has_yh))
        def _(step=step):
            padded[step, 2 : planes + 2, rows_y + 8 : rows_y + 16] = zero_rows

    head[...] = jnp.zeros(head.shape, jnp.float32)
    tail[...] = jnp.zeros(tail.shape, jnp.float32)
    squares[...] = jnp.zeros(squares.shape, jnp.float32)
    proj[...] = jnp.zeros(proj.shape, jnp.float32)
    def halo_copies(step):
        own = pl.ds(2, planes)
        inside = slice(8, rows_y + 8)
        refs = (
            (0, padded.at[step, planes + 1, inside], padded.at[step, 1, inside]),
            (0, padded.at[step, planes, inside], padded.at[step, 0, inside]),
            (1, padded.at[step, 2, inside], padded.at[step, planes + 2, inside]),
            (2, padded.at[step, own, rows_y : rows_y + 8], padded.at[step, own, 0:8]),
            (3, padded.at[step, own, 8:16], padded.at[step, own, rows_y + 8 : rows_y + 16]),
        )
        return [
            (
                sides[side][0],
                (has_xl, has_xh, has_yl, has_yh)[side],
                pltpu.make_async_remote_copy(
                    src_ref=src, dst_ref=dst,
                    send_sem=halo_send.at[step, n], recv_sem=halo_recv.at[step, n],
                    device_id=sides[side][1], device_id_type=MESH,
                ),
            )
            for n, (side, src, dst) in enumerate(refs)
        ]

    def start_halo(step, which, where=None):
        copies = halo_copies(step)
        for n in which:
            there, _, copy = copies[n]

            @pl.when(there if where is None else there & where)
            def _(copy=copy):
                copy.start()

    def wait_halo(step, which, where=None):
        copies = halo_copies(step)
        for n in which:
            _, arrives, copy = copies[n]

            @pl.when(arrives if where is None else arrives & where)
            def _(copy=copy):
                copy.wait_recv()

    def drain_halo(step):
        for there, _, copy in halo_copies(step):
            @pl.when(there)
            def _(copy=copy):
                copy.wait_send()

    stage1 = (slots1, me1, n1, member1, send1, recv1)
    stage2 = (slots2, me2, n2, member2, send2, recv2)

    def exchange(stage, begin):
        slots, me, count, member, send, recv = stage

        def copy_of(slot, d):
            return pltpu.make_async_remote_copy(
                src_ref=slots.at[slot], dst_ref=slots.at[slot],
                send_sem=send.at[d - 1], recv_sem=recv.at[slot],
                device_id=member(d)[1], device_id_type=MESH,
            )

        if begin:
            for d in range(1, count):
                copy_of(me, d).start()
            return None
        for d in range(1, count):
            copy_of(member(d)[0], d).wait_recv()
        for d in range(1, count):
            copy_of(me, d).wait_send()
        return [slots[slot] for slot in range(count)]

    def begin_sum(rnd, row):
        slots[rnd, me] = row
        for d in range(1, devices):
            pltpu.make_async_remote_copy(
                src_ref=slots.at[rnd, me], dst_ref=slots.at[rnd, me],
                send_sem=sends.at[rnd], recv_sem=recvs.at[rnd],
                device_id=member(d), device_id_type=MESH,
            ).start()

    def every(rnd):
        return pltpu.make_async_remote_copy(
            src_ref=slots.at[rnd, 0 : devices - 1], dst_ref=slots.at[rnd, 0 : devices - 1],
            send_sem=sends.at[rnd], recv_sem=recvs.at[rnd],
            device_id=member(1), device_id_type=MESH,
        )

    def finish_sum(rnd):
        every(rnd).wait_recv()
        total, rest = exact_tree([slots[rnd, slot] for slot in range(devices)])
        return total / cells, rest / cells

    shape = (padded_count, 128)
    lane = lax.broadcasted_iota(jnp.int32, shape, 1)
    sub = lax.broadcasted_iota(jnp.int32, shape, 0)
    eye = lane == sub
    eye_high = lane == sub + 64
    lane8 = lax.broadcasted_iota(jnp.int32, (8, 128), 1)
    sub8 = lax.broadcasted_iota(jnp.int32, (8, 128), 0)

    def lane_sum(values):
        return jnp.broadcast_to(jnp.sum(values, axis=1, keepdims=True), values.shape)

    def to_column(row, where=eye):
        return lane_sum(jnp.where(where, jnp.broadcast_to(row, shape), 0.0))

    def to_row(column, where=eye):
        return jnp.sum(jnp.where(where, column, 0.0), axis=0, keepdims=True)

    def project(read, count, kind, spans, fresh, square=False):
        every_one = count + square
        for first in range(0, every_one, 20):
            group = range(first, min(first + 20, every_one))

            def step(r, sums):
                at = pl.ds(pl.multiple_of(r * 8, 8), 8)
                other = read(at)
                return tuple(
                    acc + fold_lanes((vecs[i, at, :] if i < count else other) * other)
                    for i, acc in zip(group, sums)
                )

            if fresh:
                sums = (jnp.zeros((8, 128), jnp.float32),) * len(group)
            else:
                sums = tuple(proj[kind, i] for i in group)
            for start, length in spans:
                base = start // 8
                sums = lax.fori_loop(0, length // 8, lambda r, s: step(base + r, s), sums, unroll=4)
            for i, acc in zip(group, sums):
                proj[kind, i] = acc

    def projected(kind):
        return lane_sum(jnp.sum(proj[kind], axis=1))

    def stencil(step, part):
        tall = 16
        lanes = lax.broadcasted_iota(jnp.int32, (tall, width), 1)
        sx, sy, sz = WIND_SPEEDS
        centre = 6.0 + 1.5 * (sx + sy + sz)

        def piece(p, q):
            base = pl.multiple_of(q * tall, 8)
            at = pl.ds(pl.multiple_of(base + 8, 8), tall)
            block = padded[step, p + 2, pl.ds(base, tall + 16), :]
            here = block[8 : tall + 8]
            out_at = pl.ds(pl.multiple_of(p * rows_y + base, 8), tall)
            total = -(react[out_at, :] + centre) * here
            total = total + padded[step, p + 3, at, :]
            total = total + (1.0 + 2.0 * sx) * padded[step, p + 1, at, :]
            total = total - (0.5 * sx) * padded[step, p, at, :]
            total = total + roll(block, tall + 15, 0)[8 : tall + 8]
            total = total + (1.0 + 2.0 * sy) * roll(block, 1, 0)[8 : tall + 8]
            total = total - (0.5 * sy) * roll(block, 2, 0)[8 : tall + 8]
            total = total + jnp.where(lanes < width - 1, roll(here, width - 1, 1), 0.0)
            total = total + (1.0 + 2.0 * sz) * jnp.where(lanes >= 1, roll(here, 1, 1), 0.0)
            total = total - (0.5 * sz) * jnp.where(lanes >= 2, roll(here, 2, 1), 0.0)
            image[out_at, :] = total

        for p in part:
            @pl.loop(0, rows_y // tall, unroll=True)
            def _(q, p=p):
                piece(p, q)

    def widen(values):
        return jnp.concatenate([values] * (width // 128), axis=1)

    def combine(step, count, scale, inverse=None):
        tall = next(t for t in (64, 32, 16, 8) if rows_y % t == 0)
        scale_row = widen(scale)
        more = step < STEPS - 1

        def plane(p):
            @pl.loop(0, rows_y // tall)
            def _(q):
                at = pl.ds(pl.multiple_of(p * rows_y + q * tall, 8), tall)
                total = image[at, :] * scale_row
                for i in range(count):
                    total = total - coef[i : i + 1, :] * vecs[i, at, :]
                if more:
                    vecs[keep + step, at, :] = total
                    padded[step + 1, p + 2, pl.ds(pl.multiple_of(q * tall + 8, 8), tall), :] = total
                else:
                    w_out[step, at, :] = total * widen(inverse)
                    if step > 0:
                        w_out[step - 1, at, :] = vecs[keep + step - 1, at, :] * scale_row

        for p_even, p_odd, n_even, n_odd in (
            (0, planes - 1, 2, 0),
            (planes - 1, planes - 2, 0, 1),
            (planes - 2, 0, 1, 2),
        ):
            plane(jnp.where(even, p_even, p_odd))
            if more:
                start_halo(step + 1, (n_even,), even)
                start_halo(step + 1, (n_odd,), odd)
        for p in range(1, planes - 2):
            plane(p)
        if more:
            start_halo(step + 1, (3, 4))

    def outer(a, b):
        return lax.dot_general(
            a, b, (((1,), (1,)), ((), ())), preferred_element_type=jnp.float32
        )

    cut = head.shape[1]
    late = keep * 8 - 128

    def gram_block(r):
        at = pl.ds(pl.multiple_of(r, 8), 8)
        values = vecs[0:keep, at, :].reshape(keep * 8, width)
        power = values * values
        squares[...] = squares[...] + power[:, :128] + power[:, 128:]
        high = values.astype(jnp.bfloat16)
        low = (values - high.astype(jnp.float32)).astype(jnp.bfloat16)
        left = jnp.concatenate([high[:cut] * 0.5, high[cut:]], axis=0)
        first = outer(left, high[:cut]) + outer(low, high[:cut])
        second = outer(low, high[late:])
        third = outer(high[cut:] * 0.5, high[late:])
        return first, second, third

    @pl.loop(0, chunks)
    def _(c):
        @pl.when(c == 1)
        def _():
            pl.semaphore_wait(barrier, expected)
            for d in range(1, n2):
                pl.semaphore_signal(ready, inc=1, device_id=member2(d)[1], device_id_type=MESH)
            for copy in last_copies:
                copy.wait()
            start_halo(0, (2, 0, 1), even)
            start_halo(0, (0, 1, 2), odd)
            start_halo(0, (3, 4))

        load(c).wait()
        found = [gram_block(c * CHUNK + s) for s in range(0, CHUNK, 8)]
        first, second, third = (functools.reduce(lambda a, b: a + b, f) for f in zip(*found))
        head[...] = head[...] + first
        tail[...] = tail[...] + second
        tail[cut:, :] = tail[cut:, :] + third

    def picked(values, start):
        row = lax.broadcasted_iota(jnp.int32, values.shape, 0)
        column = lax.broadcasted_iota(jnp.int32, values.shape, 1)
        use = (lax.rem(row, 8) == lax.rem(column, 8)) & (column + start >= (cut if start else 0))
        kept = jnp.where(use, values, 0.0)
        return jnp.sum(kept.reshape(keep, 8, values.shape[1]), axis=1)

    spread = jnp.concatenate([picked(head[...], 0), picked(tail[...], late)], axis=1)
    place = lax.broadcasted_iota(jnp.int32, (cut + 128, 128), 0)
    place = jnp.where(place < cut, place, place - cut + late) // 8
    choose = jnp.where(place == lax.broadcasted_iota(jnp.int32, place.shape, 1), 1.0, 0.0)
    choose = choose.astype(jnp.bfloat16)
    half = jnp.zeros((keep, 128), jnp.float32)
    for _ in range(3):
        term = spread.astype(jnp.bfloat16)
        spread = spread - term.astype(jnp.float32)
        half = half + jnp.dot(term, choose, preferred_element_type=jnp.float32)
    diagonal = jnp.sum(jnp.sum(squares[...].reshape(keep, 8, 128), axis=1), axis=1, keepdims=True)
    lane_k = lax.broadcasted_iota(jnp.int32, (keep, 128), 1)
    sub_k = lax.broadcasted_iota(jnp.int32, (keep, 128), 0)
    image[0:128, 0:128] = jnp.zeros((128, 128), jnp.float32)
    image[0:keep, 0:128] = half
    turned = jnp.transpose(image[0:128, 0:128])
    pack[...] = jnp.zeros(pack.shape, jnp.float32)
    pack[0:keep] = jnp.where(lane_k == sub_k, diagonal, half + turned[0:keep])
    band = slots1.shape[1]
    folded = jnp.zeros((band, 128), jnp.float32)
    bands = [(g, g * band, min(g * band + band, padded_count)) for g in range(-(-padded_count // band))]
    for g, start, stop in bands:
        part = pack[start:stop]
        if stop - start < band:
            part = jnp.concatenate([part, jnp.zeros((band - stop + start, 128), jnp.float32)], axis=0)
        folded = folded + (roll(part, g * padded_count, 1) if g else part)
    slots1[me1] = folded

    def unfold(values):
        parts = [
            (roll(values, 128 - g * padded_count, 1) if g else values)[0 : stop - start]
            for g, start, stop in bands
        ]
        return jnp.where(lane < padded_count, jnp.concatenate(parts, axis=0), 0.0)

    def finish_gram():
        total, rest = exact_tree(exchange(stage2, False))
        row = lax.broadcasted_iota(jnp.int32, total.shape, 0)
        column = lax.broadcasted_iota(jnp.int32, total.shape, 1)
        ones = jnp.zeros(total.shape, jnp.float32)
        for g, start, _ in bands:
            on = (column == row + start + g * padded_count) & (row + start < keep)
            ones = jnp.where(on, cells, ones)
        return unfold(((ones - total) - rest) / cells)

    react_copy.wait()
    exchange(stage1, True)

    everything = [(0, rows)]

    def span(p, n=1):
        return [(p * rows_y, n * rows_y)]

    def edge(step, p):
        stencil(step, [p])
        project(lambda at: image[at, :], keep + step, 0, span(p), False, step == STEPS - 1)

    def emit(step, scale):
        scale_row = widen(scale)

        @pl.loop(0, rows // 32)
        def _(q):
            at = pl.ds(pl.multiple_of(q * 32, 32), 32)
            w_out[step, at, :] = vecs[keep + step, at, :] * scale_row

    gap = None
    scales = jnp.ones(shape, jnp.float32)
    scales_row = jnp.ones((1, 128), jnp.float32)
    lane1 = lax.broadcasted_iota(jnp.int32, (1, 128), 1)
    hess = jnp.zeros((8, 128), jnp.float32)
    b_row = jnp.zeros((1, 128), jnp.float32)
    scale = jnp.ones((1, 128), jnp.float32)
    inverse = None
    for step in range(STEPS):
        count = keep + step
        last = count - 1
        if step > 0:
            project(lambda at: vecs[last, at, :], count, 1, everything, True)
            b_row = to_row(projected(1), eye_high)
        wait_halo(step, (3, 4))
        stencil(step, range(2, planes - 1))
        project(lambda at: image[at, :], count, 0, span(2, planes - 3), True, step == STEPS - 1)
        if step > 1:
            emit(step - 2, scale)
        wait_halo(step, (0,))
        edge(step, 1)
        for p_even, p_odd, n_even, n_odd in ((0, planes - 1, 1, 2), (planes - 1, 0, 2, 1)):
            wait_halo(step, (n_even,), even)
            wait_halo(step, (n_odd,), odd)
            edge(step, jnp.where(even, p_even, p_odd))
        row = to_row(projected(0)) + b_row
        if step == 0:
            pl.semaphore_wait(ready, n2 - 1)
        begin_sum(step, row)
        if step == 0:
            slots2[me2] = tree(exchange(stage1, False))
            exchange(stage2, True)
            gap = finish_gram()
            total, rest = finish_sum(0)
        else:
            total, rest = finish_sum(step)
            overlap = to_column(total, eye_high)
            length = overlap[last : last + 1]
            length_rest = lane_sum(jnp.where(lane1 == 64 + last, rest, 0.0))
            norm = jnp.sqrt(length + EPSILON)
            scale = 1.0 / norm
            hess = jnp.where((sub8 == step - 1) & (lane8 == last), norm, hess)
            scales = jnp.where(sub == last, scale, scales)
            scales_row = jnp.where(lane1 == last, scale, scales_row)
            square, square_rest = two_product(scale, scale)
            unit, unit_rest = two_product(length, square)
            own = (((1.0 - unit) - unit_rest) - length * square_rest) - length_rest * square
            column = jnp.where(sub < last, -overlap * scales * scale, 0.0)
            column = jnp.where(sub == last, own, column)
            gap = jnp.where(sub == last, to_row(column), gap)
            gap = jnp.where(lane == last, column, gap)
        first = jnp.where(sub < count, to_column(total) * scales * scale, 0.0)
        second = lane_sum(gap * to_row(first))
        weights = jnp.where(sub < count, first + second, 0.0)
        scaled = weights * scales
        coef[...] = widen(scaled)
        if step == STEPS - 1:
            parts, parts_rest = two_product(total, scales_row)
            parts_rest = parts_rest + rest * scales_row
            power, power_rest = two_product(parts, parts)
            power_rest = power_rest + 2.0 * parts * parts_rest
            whole = jnp.where(lane1 == count, total, 0.0)
            power = jnp.where(lane1 < count, power, -whole)
            power_rest = jnp.where(lane1 < count, power_rest, jnp.where(lane1 == count, -rest, 0.0))
            grid = lane_sum(whole) * 128.0
            coarse = (power + grid) - grid
            left = -(lane_sum(coarse) + lane_sum((power - coarse) + power_rest))
            third = lane_sum(gap * to_row(second))
            left = left * scale * scale - jnp.sum(first * second + weights * third, axis=0, keepdims=True)
            norm = jnp.sqrt(jnp.maximum(left, 0.0) + EPSILON)
            inverse = 1.0 / norm
            hess = jnp.where((sub8 == step) & (lane8 == count), norm, hess)
        combine(step, count, scale, inverse)
        hess = jnp.where((sub8 == step) & (lane8 < count), to_row(weights), hess)

    h_out[...] = hess
    for step in range(STEPS):
        drain_halo(step)
        every(step).wait_send()


def group_of(count):
    for size in (4, 2):
        if count % size == 0:
            return size
    return 1


def body(basis_vectors, reaction):
    keep, planes, rows_y, width = basis_vectors.shape
    n_gx, n_gy = lax.axis_size("gx"), lax.axis_size("gy")
    g1 = group_of(n_gx)
    n1, n2 = g1 * n_gy, n_gx // g1
    size = keep + STEPS
    padded_count = -(-size // 8) * 8
    rows = planes * rows_y
    rounds = STEPS
    band = -(-padded_count // (128 // padded_count) // 8) * 8
    f32 = jnp.float32
    dma = pltpu.SemaphoreType.DMA
    held = [
        pltpu.with_memory_space_constraint(x, pltpu.HBM)
        for x in (basis_vectors.reshape(keep, rows, width), reaction.reshape(rows, width))
    ]
    w, h = pl.pallas_call(
        functools.partial(kernel, keep, planes, rows_y, n_gx, n_gy, g1),
        out_shape=(
            jax.ShapeDtypeStruct((STEPS, rows, width), f32),
            jax.ShapeDtypeStruct((8, 128), f32),
        ),
        in_specs=[pl.BlockSpec(memory_space=pltpu.HBM)] * 2,
        out_specs=(pl.BlockSpec(memory_space=pltpu.VMEM),) * 2,
        scratch_shapes=[
            pltpu.VMEM((size, rows, width), f32),
            pltpu.VMEM((STEPS, planes + 3, rows_y + 16, width), f32),
            pltpu.VMEM((rows, width), f32),
            pltpu.VMEM((rows, width), f32),
            pltpu.VMEM((keep * 8, 256), f32),
            pltpu.VMEM((keep * 8, 128), f32),
            pltpu.VMEM((keep * 8, 128), f32),
            pltpu.VMEM((padded_count, 128), f32),
            pltpu.VMEM((2, padded_count, 8, 128), f32),
            pltpu.VMEM((n1, band, 128), f32),
            pltpu.VMEM((n2, band, 128), f32),
            pltpu.VMEM((rounds, n_gx * n_gy, 1, 128), f32),
            pltpu.VMEM((padded_count, width), f32),
            dma((rows // CHUNK,)),
            dma((planes,)),
            dma,
            dma((STEPS, 5)),
            dma((STEPS, 5)),
            dma((n1,)),
            dma((n1,)),
            dma((n2,)),
            dma((n2,)),
            dma((rounds,)),
            dma((rounds,)),
            pltpu.SemaphoreType.REGULAR,
        ],
        compiler_params=pltpu.CompilerParams(
            collective_id=0, has_side_effects=True, vmem_limit_bytes=48 * 1024 * 1024
        ),
    )(*held)
    return w.reshape(STEPS, planes, rows_y, width), h[:STEPS, :size].T


def solution(mesh):
    in_specs = (P(None, "gx", "gy", None), P("gx", "gy", None))
    out_specs = (P(None, "gx", "gy", None), P())
    return jax.shard_map(body, mesh=mesh, in_specs=in_specs, out_specs=out_specs, check_vma=False)
```

```python
import functools

import jax
import jax.numpy as jnp
from jax import lax
from jax.experimental import pallas as pl
from jax.experimental.pallas import tpu as pltpu
from jax.sharding import PartitionSpec as P

STEPS = 4
WIND_SPEEDS = (0.9, 0.6, 0.4)
EPSILON = 1e-06
MESH = pl.DeviceIdType.MESH
CHUNK = 32


def roll(values, shift, axis):
    return pltpu.roll(values, shift, axis)


def fold_lanes(values):
    parts = [values[:, s : s + 128] for s in range(0, values.shape[1], 128)]
    return functools.reduce(lambda a, b: a + b, parts)


def tree(parts):
    while len(parts) > 1:
        parts = [
            parts[i] + parts[i + 1] if i + 1 < len(parts) else parts[i]
            for i in range(0, len(parts), 2)
        ]
    return parts[0]


def two_sum(a, b):
    total = a + b
    other = total - a
    return total, (a - (total - other)) + (b - other)


def halves(a):
    scaled = a * 4097.0
    high = scaled - (scaled - a)
    return high, a - high


def two_product(a, b):
    product = a * b
    ah, al = halves(a)
    bh, bl = halves(b)
    return product, ((ah * bh - product) + ah * bl + al * bh) + al * bl


def exact_tree(parts):
    def add(a, b):
        total, rest = two_sum(a[0], b[0])
        return total, (a[1] + b[1]) + rest

    pairs = [(part, jnp.zeros_like(part)) for part in parts]
    while len(pairs) > 1:
        pairs = [
            add(pairs[i], pairs[i + 1]) if i + 1 < len(pairs) else pairs[i]
            for i in range(0, len(pairs), 2)
        ]
    return pairs[0]


def kernel(
    keep, planes, rows_y, n_gx, n_gy, g1,
    basis, reaction, w_out, h_out,
    vecs, padded, image, react, head, tail, squares, pack, proj, slots1, slots2, slots, coef,
    load_sem, last_sem, react_sem,
    halo_send, halo_recv, send1, recv1, send2, recv2, sends, recvs, ready,
):
    width = basis.shape[2]
    rows = planes * rows_y
    padded_count = proj.shape[1]
    gx = lax.axis_index("gx")
    gy = lax.axis_index("gy")
    n1 = n_gy * g1
    n2 = n_gx // g1
    low = lax.rem(gx, g1)
    high = gx // g1
    me1 = gy * g1 + low
    me2 = high
    cells = float(rows * width * n_gx * n_gy)

    last_copies = [
        pltpu.make_async_copy(
            basis.at[keep - 1, p * rows_y : (p + 1) * rows_y],
            padded.at[0, p + 2, 8 : rows_y + 8],
            last_sem.at[p],
        )
        for p in range(planes)
    ]
    for copy in last_copies:
        copy.start()
    chunks = rows // CHUNK

    def load(c):
        at = pl.ds(pl.multiple_of(c * CHUNK, CHUNK), CHUNK)
        return pltpu.make_async_copy(basis.at[:, at], vecs.at[0:keep, at], load_sem.at[c])

    @pl.loop(0, chunks)
    def _(c):
        load(c).start()

    react_copy = pltpu.make_async_copy(reaction, react, react_sem)
    react_copy.start()

    has_xl, has_xh = gx > 0, gx < n_gx - 1
    has_yl, has_yh = gy > 0, gy < n_gy - 1

    def member1(d):
        p = lax.rem(me1 + d, n1)
        return p, {"gx": high * g1 + lax.rem(p, g1), "gy": p // g1}

    def member2(d):
        p = lax.rem(me2 + d, n2)
        return p, {"gx": p * g1 + low, "gy": gy}

    me = gx * n_gy + gy
    devices = n_gx * n_gy

    bits = devices.bit_length() - 1
    turns = [(1 - 2 * lax.rem(me // 2**i, 2)) * 2**i for i in range(bits)]

    def member(d):
        if devices == 2**bits:
            p = me + functools.reduce(lambda a, b: a + b, [t for i, t in enumerate(turns) if d >> i & 1])
        else:
            p = lax.rem(me + d, devices)
        return {"gx": p // n_gy, "gy": lax.rem(p, n_gy)}

    barrier = pltpu.get_barrier_semaphore()
    for d in range(1, n1):
        pl.semaphore_signal(barrier, inc=1, device_id=member1(d)[1], device_id_type=MESH)
    for d in range(1, n2):
        pl.semaphore_signal(barrier, inc=1, device_id=member2(d)[1], device_id_type=MESH)
    sides = (
        (has_xh, {"gx": gx + 1, "gy": gy}),
        (has_xl, {"gx": gx - 1, "gy": gy}),
        (has_yh, {"gx": gx, "gy": gy + 1}),
        (has_yl, {"gx": gx, "gy": gy - 1}),
    )
    even = lax.rem(gx, 2) == 0
    odd = jnp.logical_not(even)
    expected = n1 - 1 + n2 - 1
    for there, device in sides:
        @pl.when(there)
        def _(device=device):
            pl.semaphore_signal(barrier, inc=1, device_id=device, device_id_type=MESH)

        expected = expected + there.astype(jnp.int32)

    zero_plane = jnp.zeros((1, rows_y, width), jnp.float32)
    zero_rows = jnp.zeros((planes, 8, width), jnp.float32)
    for step in range(STEPS):
        @pl.when(jnp.logical_not(has_xl))
        def _(step=step):
            padded[step, 0:1, 8 : rows_y + 8] = zero_plane
            padded[step, 1:2, 8 : rows_y + 8] = zero_plane

        @pl.when(jnp.logical_not(has_xh))
        def _(step=step):
            padded[step, planes + 2 : planes + 3, 8 : rows_y + 8] = zero_plane

        @pl.when(jnp.logical_not(has_yl))
        def _(step=step):
            padded[step, 2 : planes + 2, 0:8] = zero_rows

        @pl.when(jnp.logical_not(has_yh))
        def _(step=step):
            padded[step, 2 : planes + 2, rows_y + 8 : rows_y + 16] = zero_rows

    head[...] = jnp.zeros(head.shape, jnp.float32)
    tail[...] = jnp.zeros(tail.shape, jnp.float32)
    squares[...] = jnp.zeros(squares.shape, jnp.float32)
    proj[...] = jnp.zeros(proj.shape, jnp.float32)
    rows_half = rows_y // 2

    def halo_copies(step):
        own = pl.ds(2, planes)
        part = [slice(8 + h * rows_half, 8 + (h + 1) * rows_half) for h in range(2)]
        refs = [
            (side, padded.at[step, src, at], padded.at[step, dst, at])
            for side, src, dst in ((0, planes + 1, 1), (0, planes, 0), (1, 2, planes + 2))
            for at in part
        ] + [
            (2, padded.at[step, own, rows_y : rows_y + 8], padded.at[step, own, 0:8]),
            (3, padded.at[step, own, 8:16], padded.at[step, own, rows_y + 8 : rows_y + 16]),
        ]
        return [
            (
                sides[side][0],
                (has_xl, has_xh, has_yl, has_yh)[side],
                pltpu.make_async_remote_copy(
                    src_ref=src, dst_ref=dst,
                    send_sem=halo_send.at[step, n], recv_sem=halo_recv.at[step, n],
                    device_id=sides[side][1], device_id_type=MESH,
                ),
            )
            for n, (side, src, dst) in enumerate(refs)
        ]

    def start_halo(step, which, where=None):
        copies = halo_copies(step)
        for n in which:
            there, _, copy = copies[n]

            @pl.when(there if where is None else there & where)
            def _(copy=copy):
                copy.start()

    def wait_halo(step, which, where=None):
        copies = halo_copies(step)
        for n in which:
            _, arrives, copy = copies[n]

            @pl.when(arrives if where is None else arrives & where)
            def _(copy=copy):
                copy.wait_recv()

    def drain_halo(step):
        for there, _, copy in halo_copies(step):
            @pl.when(there)
            def _(copy=copy):
                copy.wait_send()

    stage1 = (slots1, me1, n1, member1, send1, recv1)
    stage2 = (slots2, me2, n2, member2, send2, recv2)

    def exchange(stage, begin):
        slots, me, count, member, send, recv = stage

        def copy_of(slot, d):
            return pltpu.make_async_remote_copy(
                src_ref=slots.at[slot], dst_ref=slots.at[slot],
                send_sem=send.at[d - 1], recv_sem=recv.at[slot],
                device_id=member(d)[1], device_id_type=MESH,
            )

        if begin:
            for d in range(1, count):
                copy_of(me, d).start()
            return None
        for d in range(1, count):
            copy_of(member(d)[0], d).wait_recv()
        for d in range(1, count):
            copy_of(me, d).wait_send()
        return [slots[slot] for slot in range(count)]

    def begin_sum(rnd, row):
        slots[rnd, me] = row
        for d in range(devices - 1, 0, -1):
            pltpu.make_async_remote_copy(
                src_ref=slots.at[rnd, me], dst_ref=slots.at[rnd, me],
                send_sem=sends.at[rnd], recv_sem=recvs.at[rnd],
                device_id=member(d), device_id_type=MESH,
            ).start()

    def every(rnd):
        return pltpu.make_async_remote_copy(
            src_ref=slots.at[rnd, 0 : devices - 1], dst_ref=slots.at[rnd, 0 : devices - 1],
            send_sem=sends.at[rnd], recv_sem=recvs.at[rnd],
            device_id=member(1), device_id_type=MESH,
        )

    def finish_sum(rnd):
        every(rnd).wait_recv()
        total, rest = exact_tree([slots[rnd, slot] for slot in range(devices)])
        return total / cells, rest / cells

    shape = (padded_count, 128)
    lane = lax.broadcasted_iota(jnp.int32, shape, 1)
    sub = lax.broadcasted_iota(jnp.int32, shape, 0)
    eye = lane == sub
    eye_high = lane == sub + 64
    lane8 = lax.broadcasted_iota(jnp.int32, (8, 128), 1)
    sub8 = lax.broadcasted_iota(jnp.int32, (8, 128), 0)

    def lane_sum(values):
        return jnp.broadcast_to(jnp.sum(values, axis=1, keepdims=True), values.shape)

    def to_column(row, where=eye):
        return lane_sum(jnp.where(where, jnp.broadcast_to(row, shape), 0.0))

    def to_row(column, where=eye):
        return jnp.sum(jnp.where(where, column, 0.0), axis=0, keepdims=True)

    def project(read, count, kind, spans, fresh, square=False):
        every_one = count + square
        for first in range(0, every_one, 20):
            group = range(first, min(first + 20, every_one))

            def step(r, sums):
                at = pl.ds(pl.multiple_of(r * 8, 8), 8)
                other = read(at)
                return tuple(
                    acc + fold_lanes((vecs[i, at, :] if i < count else other) * other)
                    for i, acc in zip(group, sums)
                )

            if fresh:
                sums = (jnp.zeros((8, 128), jnp.float32),) * len(group)
            else:
                sums = tuple(proj[kind, i] for i in group)
            for start, length in spans:
                base = start // 8
                sums = lax.fori_loop(0, length // 8, lambda r, s: step(base + r, s), sums, unroll=4)
            for i, acc in zip(group, sums):
                proj[kind, i] = acc

    def project_late(step, count, p, halo, factor, h):
        square = step == STEPS - 1
        every_one = count + square
        for first in range(0, every_one, 20):
            group = range(first, min(first + 20, every_one))

            def add(r, sums):
                at = pl.ds(pl.multiple_of(p * rows_y + h * rows_half + r * 8, 8), 8)
                other = padded[step, halo, pl.ds(pl.multiple_of(8 + h * rows_half + r * 8, 8), 8), :] * factor
                whole = other
                if every_one in (group.stop,):
                    whole = image[at, :] + other
                    image[at, :] = whole
                return tuple(
                    acc + fold_lanes(vecs[i, at, :] * other if i < count else whole * whole)
                    for i, acc in zip(group, sums)
                )

            sums = lax.fori_loop(0, rows_half // 8, add, tuple(proj[0, i] for i in group), unroll=True)
            for i, acc in zip(group, sums):
                proj[0, i] = acc

    def projected(kind):
        return lane_sum(jnp.sum(proj[kind], axis=1))

    def stencil(step, part):
        tall = 16
        lanes = lax.broadcasted_iota(jnp.int32, (tall, width), 1)
        sx, sy, sz = WIND_SPEEDS
        centre = 6.0 + 1.5 * (sx + sy + sz)

        def piece(p, q):
            base = pl.multiple_of(q * tall, 8)
            at = pl.ds(pl.multiple_of(base + 8, 8), tall)
            block = padded[step, p + 2, pl.ds(base, tall + 16), :]
            here = block[8 : tall + 8]
            out_at = pl.ds(pl.multiple_of(p * rows_y + base, 8), tall)
            total = -(react[out_at, :] + centre) * here
            total = total + padded[step, p + 3, at, :] if p < planes - 1 else total
            total = total + (1.0 + 2.0 * sx) * padded[step, p + 1, at, :]
            total = total - (0.5 * sx) * padded[step, p, at, :] if p > 0 else total
            total = total + roll(block, tall + 15, 0)[8 : tall + 8]
            total = total + (1.0 + 2.0 * sy) * roll(block, 1, 0)[8 : tall + 8]
            total = total - (0.5 * sy) * roll(block, 2, 0)[8 : tall + 8]
            total = total + jnp.where(lanes < width - 1, roll(here, width - 1, 1), 0.0)
            total = total + (1.0 + 2.0 * sz) * jnp.where(lanes >= 1, roll(here, 1, 1), 0.0)
            total = total - (0.5 * sz) * jnp.where(lanes >= 2, roll(here, 2, 1), 0.0)
            image[out_at, :] = total

        for p in part:
            @pl.loop(0, rows_y // tall, unroll=True)
            def _(q, p=p):
                piece(p, q)

    def widen(values):
        return jnp.concatenate([values] * (width // 128), axis=1)

    def combine(step, count, scale, inverse=None):
        scale_row = widen(scale)
        more = step < STEPS - 1

        def plane(p, start, tall):
            at = pl.ds(pl.multiple_of(p * rows_y + start, 8), tall)
            total = image[at, :] * scale_row
            for i in range(count):
                total = total - coef[i : i + 1, :] * vecs[i, at, :]
            if more:
                vecs[keep + step, at, :] = total
                padded[step + 1, p + 2, start + 8 : start + 8 + tall, :] = total
            else:
                w_out[step, at, :] = total * widen(inverse)
                if step > 0:
                    w_out[step - 1, at, :] = vecs[keep + step - 1, at, :] * scale_row

        for n, (p_even, p_odd, n_even, n_odd) in enumerate((
            (0, planes - 1, 4, 0),
            (planes - 1, planes - 2, 0, 2),
            (planes - 2, 0, 2, 4),
        )):
            p = jnp.where(even, p_even, p_odd)
            if n > 0:
                plane(p, 0, rows_y)
            for h in range(2):
                if n == 0:
                    plane(p, h * rows_half, rows_half)
                if more:
                    start_halo(step + 1, (n_even + h,), even)
                    start_halo(step + 1, (n_odd + h,), odd)
        for p in range(1, planes - 2):
            plane(p, 0, rows_y)
        if more:
            start_halo(step + 1, (6, 7))

    def outer(a, b):
        return lax.dot_general(
            a, b, (((1,), (1,)), ((), ())), preferred_element_type=jnp.float32
        )

    cut = head.shape[1]
    late = keep * 8 - 128

    def gram_block(r):
        at = pl.ds(pl.multiple_of(r, 8), 8)
        values = vecs[0:keep, at, :].reshape(keep * 8, width)
        power = values * values
        squares[...] = squares[...] + power[:, :128] + power[:, 128:]
        high = values.astype(jnp.bfloat16)
        low = (values - high.astype(jnp.float32)).astype(jnp.bfloat16)
        left = jnp.concatenate([high[:cut] * 0.5, high[cut:]], axis=0)
        first = outer(left, high[:cut]) + outer(low, high[:cut])
        second = outer(low, high[late:])
        third = outer(high[cut:] * 0.5, high[late:])
        return first, second, third

    @pl.loop(0, chunks)
    def _(c):
        @pl.when(c == 1)
        def _():
            pl.semaphore_wait(barrier, expected)
            for d in range(1, n2):
                pl.semaphore_signal(ready, inc=1, device_id=member2(d)[1], device_id_type=MESH)
            for copy in last_copies:
                copy.wait()
            start_halo(0, (4, 5, 0, 1, 2, 3), even)
            start_halo(0, (0, 1, 2, 3, 4, 5), odd)
            start_halo(0, (6, 7))

        load(c).wait()
        found = [gram_block(c * CHUNK + s) for s in range(0, CHUNK, 8)]
        first, second, third = (functools.reduce(lambda a, b: a + b, f) for f in zip(*found))
        head[...] = head[...] + first
        tail[...] = tail[...] + second
        tail[cut:, :] = tail[cut:, :] + third

    def picked(values, start):
        row = lax.broadcasted_iota(jnp.int32, values.shape, 0)
        column = lax.broadcasted_iota(jnp.int32, values.shape, 1)
        use = (lax.rem(row, 8) == lax.rem(column, 8)) & (column + start >= (cut if start else 0))
        kept = jnp.where(use, values, 0.0)
        return jnp.sum(kept.reshape(keep, 8, values.shape[1]), axis=1)

    spread = jnp.concatenate([picked(head[...], 0), picked(tail[...], late)], axis=1)
    place = lax.broadcasted_iota(jnp.int32, (cut + 128, 128), 0)
    place = jnp.where(place < cut, place, place - cut + late) // 8
    choose = jnp.where(place == lax.broadcasted_iota(jnp.int32, place.shape, 1), 1.0, 0.0)
    choose = choose.astype(jnp.bfloat16)
    half = jnp.zeros((keep, 128), jnp.float32)
    for _ in range(3):
        term = spread.astype(jnp.bfloat16)
        spread = spread - term.astype(jnp.float32)
        half = half + jnp.dot(term, choose, preferred_element_type=jnp.float32)
    diagonal = jnp.sum(jnp.sum(squares[...].reshape(keep, 8, 128), axis=1), axis=1, keepdims=True)
    lane_k = lax.broadcasted_iota(jnp.int32, (keep, 128), 1)
    sub_k = lax.broadcasted_iota(jnp.int32, (keep, 128), 0)
    image[0:128, 0:128] = jnp.zeros((128, 128), jnp.float32)
    image[0:keep, 0:128] = half
    turned = jnp.transpose(image[0:128, 0:128])
    pack[...] = jnp.zeros(pack.shape, jnp.float32)
    pack[0:keep] = jnp.where(lane_k == sub_k, diagonal, half + turned[0:keep])
    band = slots1.shape[1]
    folded = jnp.zeros((band, 128), jnp.float32)
    bands = [(g, g * band, min(g * band + band, padded_count)) for g in range(-(-padded_count // band))]
    for g, start, stop in bands:
        part = pack[start:stop]
        if stop - start < band:
            part = jnp.concatenate([part, jnp.zeros((band - stop + start, 128), jnp.float32)], axis=0)
        folded = folded + (roll(part, g * padded_count, 1) if g else part)
    slots1[me1] = folded

    def unfold(values):
        parts = [
            (roll(values, 128 - g * padded_count, 1) if g else values)[0 : stop - start]
            for g, start, stop in bands
        ]
        return jnp.where(lane < padded_count, jnp.concatenate(parts, axis=0), 0.0)

    def finish_gram():
        total, rest = exact_tree(exchange(stage2, False))
        row = lax.broadcasted_iota(jnp.int32, total.shape, 0)
        column = lax.broadcasted_iota(jnp.int32, total.shape, 1)
        ones = jnp.zeros(total.shape, jnp.float32)
        for g, start, _ in bands:
            on = (column == row + start + g * padded_count) & (row + start < keep)
            ones = jnp.where(on, cells, ones)
        return unfold(((ones - total) - rest) / cells)

    react_copy.wait()
    exchange(stage1, True)

    everything = [(0, rows)]

    def span(p, n=1):
        return [(p * rows_y, n * rows_y)]

    def project_image(step, spans, fresh=False, square=False):
        project(lambda at: image[at, :], keep + step, 0, spans, fresh, square)

    sx = WIND_SPEEDS[0]
    order = (
        [(0, 0, -0.5 * sx, h, 2 + h) for h in range(2)],
        [(planes - 1, planes + 2, 1.0, h, 4 + h) for h in range(2)],
    )

    def emit(step, scale):
        scale_row = widen(scale)

        @pl.loop(0, rows // 32)
        def _(q):
            at = pl.ds(pl.multiple_of(q * 32, 32), 32)
            w_out[step, at, :] = vecs[keep + step, at, :] * scale_row

    gap = None
    scales = jnp.ones(shape, jnp.float32)
    scales_row = jnp.ones((1, 128), jnp.float32)
    lane1 = lax.broadcasted_iota(jnp.int32, (1, 128), 1)
    hess = jnp.zeros((8, 128), jnp.float32)
    b_row = jnp.zeros((1, 128), jnp.float32)
    scale = jnp.ones((1, 128), jnp.float32)
    inverse = None
    for step in range(STEPS):
        count = keep + step
        last = count - 1
        if step > 0:
            project(lambda at: vecs[last, at, :], count, 1, everything, True)
            b_row = to_row(projected(1), eye_high)
        square = step == STEPS - 1
        wait_halo(step, (6, 7))
        stencil(step, range(2, planes))
        project_image(step, span(2, planes - 3), True, square)
        project_image(step, span(planes - 1))
        if step > 1:
            emit(step - 2, scale)
        wait_halo(step, (0, 1))
        stencil(step, range(2))
        project_image(step, span(0))
        project_image(step, span(1), False, square)
        for first, second in zip(order[0] + order[1], order[1] + order[0]):
            wait_halo(step, (first[4],), even)
            wait_halo(step, (second[4],), odd)
            p, halo, factor = (jnp.where(even, a, b) for a, b in zip(first[:3], second[:3]))
            project_late(step, count, p, halo, factor, first[3])
        row = to_row(projected(0)) + b_row
        if step == 0:
            pl.semaphore_wait(ready, n2 - 1)
        begin_sum(step, row)
        drain_halo(step)
        if step == 0:
            slots2[me2] = tree(exchange(stage1, False))
            exchange(stage2, True)
            gap = finish_gram()
            total, rest = finish_sum(0)
        else:
            every(step - 1).wait_send()
            total, rest = finish_sum(step)
            overlap = to_column(total, eye_high)
            length = overlap[last : last + 1]
            length_rest = lane_sum(jnp.where(lane1 == 64 + last, rest, 0.0))
            norm = jnp.sqrt(length + EPSILON)
            scale = 1.0 / norm
            hess = jnp.where((sub8 == step - 1) & (lane8 == last), norm, hess)
            scales = jnp.where(sub == last, scale, scales)
            scales_row = jnp.where(lane1 == last, scale, scales_row)
            square, square_rest = two_product(scale, scale)
            unit, unit_rest = two_product(length, square)
            own = (((1.0 - unit) - unit_rest) - length * square_rest) - length_rest * square
            column = jnp.where(sub < last, -overlap * scales * scale, 0.0)
            column = jnp.where(sub == last, own, column)
            gap = jnp.where(sub == last, to_row(column), gap)
            gap = jnp.where(lane == last, column, gap)
        first = jnp.where(sub < count, to_column(total) * scales * scale, 0.0)
        second = lane_sum(gap * to_row(first))
        weights = jnp.where(sub < count, first + second, 0.0)
        scaled = weights * scales
        coef[...] = widen(scaled)
        if step == STEPS - 1:
            parts, parts_rest = two_product(total, scales_row)
            parts_rest = parts_rest + rest * scales_row
            power, power_rest = two_product(parts, parts)
            power_rest = power_rest + 2.0 * parts * parts_rest
            whole = jnp.where(lane1 == count, total, 0.0)
            power = jnp.where(lane1 < count, power, -whole)
            power_rest = jnp.where(lane1 < count, power_rest, jnp.where(lane1 == count, -rest, 0.0))
            grid = lane_sum(whole) * 128.0
            coarse = (power + grid) - grid
            left = -(lane_sum(coarse) + lane_sum((power - coarse) + power_rest))
            third = lane_sum(gap * to_row(second))
            left = left * scale * scale - jnp.sum(first * second + weights * third, axis=0, keepdims=True)
            norm = jnp.sqrt(jnp.maximum(left, 0.0) + EPSILON)
            inverse = 1.0 / norm
            hess = jnp.where((sub8 == step) & (lane8 == count), norm, hess)
        hess = jnp.where((sub8 == step) & (lane8 < count), to_row(weights), hess)
        if step == STEPS - 1:
            h_out[...] = hess
        combine(step, count, scale, inverse)

    every(STEPS - 1).wait_send()


def group_of(count):
    for size in (4, 2):
        if count % size == 0:
            return size
    return 1


def body(basis_vectors, reaction):
    keep, planes, rows_y, width = basis_vectors.shape
    n_gx, n_gy = lax.axis_size("gx"), lax.axis_size("gy")
    g1 = group_of(n_gx)
    n1, n2 = g1 * n_gy, n_gx // g1
    size = keep + STEPS
    padded_count = -(-size // 8) * 8
    rows = planes * rows_y
    rounds = STEPS
    band = -(-padded_count // (128 // padded_count) // 8) * 8
    f32 = jnp.float32
    dma = pltpu.SemaphoreType.DMA
    held = [
        pltpu.with_memory_space_constraint(x, pltpu.HBM)
        for x in (basis_vectors.reshape(keep, rows, width), reaction.reshape(rows, width))
    ]
    w, h = pl.pallas_call(
        functools.partial(kernel, keep, planes, rows_y, n_gx, n_gy, g1),
        out_shape=(
            jax.ShapeDtypeStruct((STEPS, rows, width), f32),
            jax.ShapeDtypeStruct((8, 128), f32),
        ),
        in_specs=[pl.BlockSpec(memory_space=pltpu.HBM)] * 2,
        out_specs=(pl.BlockSpec(memory_space=pltpu.VMEM),) * 2,
        scratch_shapes=[
            pltpu.VMEM((size, rows, width), f32),
            pltpu.VMEM((STEPS, planes + 3, rows_y + 16, width), f32),
            pltpu.VMEM((rows, width), f32),
            pltpu.VMEM((rows, width), f32),
            pltpu.VMEM((keep * 8, 256), f32),
            pltpu.VMEM((keep * 8, 128), f32),
            pltpu.VMEM((keep * 8, 128), f32),
            pltpu.VMEM((padded_count, 128), f32),
            pltpu.VMEM((2, padded_count, 8, 128), f32),
            pltpu.VMEM((n1, band, 128), f32),
            pltpu.VMEM((n2, band, 128), f32),
            pltpu.VMEM((rounds, n_gx * n_gy, 1, 128), f32),
            pltpu.VMEM((padded_count, width), f32),
            dma((rows // CHUNK,)),
            dma((planes,)),
            dma,
            dma((STEPS, 8)),
            dma((STEPS, 8)),
            dma((n1,)),
            dma((n1,)),
            dma((n2,)),
            dma((n2,)),
            dma((rounds,)),
            dma((rounds,)),
            pltpu.SemaphoreType.REGULAR,
        ],
        compiler_params=pltpu.CompilerParams(
            collective_id=0, has_side_effects=True, vmem_limit_bytes=48 * 1024 * 1024
        ),
    )(*held)
    return w.reshape(STEPS, planes, rows_y, width), h[:STEPS, :size].T


def solution(mesh):
    in_specs = (P(None, "gx", "gy", None), P("gx", "gy", None))
    out_specs = (P(None, "gx", "gy", None), P())
    return jax.shard_map(body, mesh=mesh, in_specs=in_specs, out_specs=out_specs, check_vma=False)
```

```python
import functools

import jax
import jax.numpy as jnp
from jax import lax
from jax.experimental import pallas as pl
from jax.experimental.pallas import tpu as pltpu
from jax.sharding import PartitionSpec as P

STEPS = 4
WIND_SPEEDS = (0.9, 0.6, 0.4)
EPSILON = 1e-06
MESH = pl.DeviceIdType.MESH
CHUNK = 32


def roll(values, shift, axis):
    return pltpu.roll(values, shift, axis)


def fold_lanes(values):
    parts = [values[:, s : s + 128] for s in range(0, values.shape[1], 128)]
    return functools.reduce(lambda a, b: a + b, parts)


def tree(parts):
    while len(parts) > 1:
        parts = [
            parts[i] + parts[i + 1] if i + 1 < len(parts) else parts[i]
            for i in range(0, len(parts), 2)
        ]
    return parts[0]


def two_sum(a, b):
    total = a + b
    other = total - a
    return total, (a - (total - other)) + (b - other)


def halves(a):
    scaled = a * 4097.0
    high = scaled - (scaled - a)
    return high, a - high


def two_product(a, b):
    product = a * b
    ah, al = halves(a)
    bh, bl = halves(b)
    return product, ((ah * bh - product) + ah * bl + al * bh) + al * bl


def exact_tree(parts):
    def add(a, b):
        total, rest = two_sum(a[0], b[0])
        return total, (a[1] + b[1]) + rest

    pairs = [(part, jnp.zeros_like(part)) for part in parts]
    while len(pairs) > 1:
        pairs = [
            add(pairs[i], pairs[i + 1]) if i + 1 < len(pairs) else pairs[i]
            for i in range(0, len(pairs), 2)
        ]
    return pairs[0]


def kernel(
    keep, planes, rows_y, n_gx, n_gy, g1,
    basis, reaction, w_out, h_out,
    vecs, padded, image, react, head, tail, squares, pack, proj, slots1, slots2, slots, coef,
    load_sem, last_sem, react_sem,
    halo_send, halo_recv, send1, recv1, send2, recv2, sends, recvs, ready,
):
    width = basis.shape[2]
    rows = planes * rows_y
    padded_count = proj.shape[1]
    gx = lax.axis_index("gx")
    gy = lax.axis_index("gy")
    n1 = n_gy * g1
    n2 = n_gx // g1
    low = lax.rem(gx, g1)
    high = gx // g1
    me1 = gy * g1 + low
    me2 = high
    cells = float(rows * width * n_gx * n_gy)

    last_copies = [
        pltpu.make_async_copy(
            basis.at[keep - 1, p * rows_y : (p + 1) * rows_y],
            padded.at[0, p + 2, 8 : rows_y + 8],
            last_sem,
        )
        for p in range(planes)
    ]
    for copy in last_copies:
        copy.start()
    all_last = padded.at[0, 2 : planes + 2, 8 : rows_y + 8]
    chunks = rows // CHUNK

    def load(c):
        at = pl.ds(pl.multiple_of(c * CHUNK, CHUNK), CHUNK)
        return pltpu.make_async_copy(basis.at[:, at], vecs.at[0:keep, at], load_sem.at[c])

    @pl.loop(0, chunks)
    def _(c):
        load(c).start()

    react_copy = pltpu.make_async_copy(reaction, react, react_sem)
    react_copy.start()

    has_xl, has_xh = gx > 0, gx < n_gx - 1
    has_yl, has_yh = gy > 0, gy < n_gy - 1

    def member1(d):
        p = lax.rem(me1 + d, n1)
        return p, {"gx": high * g1 + lax.rem(p, g1), "gy": p // g1}

    def member2(d):
        p = lax.rem(me2 + d, n2)
        return p, {"gx": p * g1 + low, "gy": gy}

    me = gx * n_gy + gy
    devices = n_gx * n_gy

    bits = devices.bit_length() - 1
    turns = [(1 - 2 * lax.rem(me // 2**i, 2)) * 2**i for i in range(bits)]

    def member(d):
        if devices == 2**bits:
            p = me + functools.reduce(lambda a, b: a + b, [t for i, t in enumerate(turns) if d >> i & 1])
        else:
            p = lax.rem(me + d, devices)
        return {"gx": p // n_gy, "gy": lax.rem(p, n_gy)}

    barrier = pltpu.get_barrier_semaphore()
    for d in range(1, n1):
        pl.semaphore_signal(barrier, inc=1, device_id=member1(d)[1], device_id_type=MESH)
    for d in range(1, n2):
        pl.semaphore_signal(barrier, inc=1, device_id=member2(d)[1], device_id_type=MESH)
    sides = (
        (has_xh, {"gx": gx + 1, "gy": gy}),
        (has_xl, {"gx": gx - 1, "gy": gy}),
        (has_yh, {"gx": gx, "gy": gy + 1}),
        (has_yl, {"gx": gx, "gy": gy - 1}),
    )
    even = lax.rem(gx, 2) == 0
    odd = jnp.logical_not(even)
    expected = n1 - 1 + n2 - 1
    for there, device in sides:
        @pl.when(there)
        def _(device=device):
            pl.semaphore_signal(barrier, inc=1, device_id=device, device_id_type=MESH)

        expected = expected + there.astype(jnp.int32)

    zero_plane = jnp.zeros((1, rows_y, width), jnp.float32)
    zero_rows = jnp.zeros((planes, 8, width), jnp.float32)
    for step in range(STEPS):
        @pl.when(jnp.logical_not(has_xl))
        def _(step=step):
            padded[step, 0:1, 8 : rows_y + 8] = zero_plane
            padded[step, 1:2, 8 : rows_y + 8] = zero_plane

        @pl.when(jnp.logical_not(has_xh))
        def _(step=step):
            padded[step, planes + 2 : planes + 3, 8 : rows_y + 8] = zero_plane

        @pl.when(jnp.logical_not(has_yl))
        def _(step=step):
            padded[step, 2 : planes + 2, 0:8] = zero_rows

        @pl.when(jnp.logical_not(has_yh))
        def _(step=step):
            padded[step, 2 : planes + 2, rows_y + 8 : rows_y + 16] = zero_rows

    head[...] = jnp.zeros(head.shape, jnp.float32)
    tail[...] = jnp.zeros(tail.shape, jnp.float32)
    squares[...] = jnp.zeros(squares.shape, jnp.float32)
    proj[...] = jnp.zeros(proj.shape, jnp.float32)
    rows_half = rows_y // 2

    def halo_copies(step):
        own = pl.ds(2, planes)
        part = [slice(8 + h * rows_half, 8 + (h + 1) * rows_half) for h in range(2)]
        refs = [
            (side, padded.at[step, src, at], padded.at[step, dst, at])
            for side, src, dst in ((0, planes + 1, 1), (0, planes, 0), (1, 2, planes + 2))
            for at in part
        ] + [
            (2, padded.at[step, own, rows_y : rows_y + 8], padded.at[step, own, 0:8]),
            (3, padded.at[step, own, 8:16], padded.at[step, own, rows_y + 8 : rows_y + 16]),
        ]
        return [
            (
                sides[side][0],
                (has_xl, has_xh, has_yl, has_yh)[side],
                pltpu.make_async_remote_copy(
                    src_ref=src, dst_ref=dst,
                    send_sem=halo_send.at[side], recv_sem=halo_recv.at[n],
                    device_id=sides[side][1], device_id_type=MESH,
                ),
            )
            for n, (side, src, dst) in enumerate(refs)
        ]

    def start_halo(step, which, where=None):
        copies = halo_copies(step)
        for n in which:
            there, _, copy = copies[n]

            @pl.when(there if where is None else there & where)
            def _(copy=copy):
                copy.start()

    def wait_halo(step, which, where=None):
        copies = halo_copies(step)
        for n in which:
            _, arrives, copy = copies[n]

            @pl.when(arrives if where is None else arrives & where)
            def _(copy=copy):
                copy.wait_recv()

    def drain_halo(step):
        inside = slice(8, rows_y + 8)
        copies = halo_copies(step)
        groups = (
            padded.at[step, planes : planes + 2, inside],
            padded.at[step, 2:3, inside],
        )
        for side, group in enumerate(groups):
            @pl.when(sides[side][0])
            def _(side=side, group=group):
                pltpu.make_async_remote_copy(
                    src_ref=group, dst_ref=group,
                    send_sem=halo_send.at[side], recv_sem=halo_recv.at[0],
                    device_id=sides[side][1], device_id_type=MESH,
                ).wait_send()

        for there, _, copy in copies[6:]:
            @pl.when(there)
            def _(copy=copy):
                copy.wait_send()

    stage1 = (slots1, me1, n1, member1, send1, recv1)
    stage2 = (slots2, me2, n2, member2, send2, recv2)

    def exchange(stage, begin):
        slots, me, count, member, send, recv = stage

        def copy_of(at, d):
            return pltpu.make_async_remote_copy(
                src_ref=slots.at[at], dst_ref=slots.at[at], send_sem=send, recv_sem=recv,
                device_id=member(d)[1], device_id_type=MESH,
            )

        if begin:
            for d in range(1, count):
                copy_of(me, d).start()
            return None
        if count > 1:
            every_copy = copy_of(pl.ds(0, count - 1), 1)
            every_copy.wait_recv()
            every_copy.wait_send()
        return [slots[slot] for slot in range(count)]

    def begin_sum(rnd, row):
        slots[rnd, me] = row
        for d in range(devices - 1, 0, -1):
            pltpu.make_async_remote_copy(
                src_ref=slots.at[rnd, me], dst_ref=slots.at[rnd, me],
                send_sem=sends, recv_sem=recvs.at[rnd % 2],
                device_id=member(d), device_id_type=MESH,
            ).start()

    def every(rnd):
        return pltpu.make_async_remote_copy(
            src_ref=slots.at[rnd, 0 : devices - 1], dst_ref=slots.at[rnd, 0 : devices - 1],
            send_sem=sends, recv_sem=recvs.at[rnd % 2],
            device_id=member(1), device_id_type=MESH,
        )

    def finish_sum(rnd):
        every(rnd).wait_recv()
        every(rnd).wait_send()
        total, rest = exact_tree([slots[rnd, slot] for slot in range(devices)])
        return total / cells, rest / cells

    shape = (padded_count, 128)
    lane = lax.broadcasted_iota(jnp.int32, shape, 1)
    sub = lax.broadcasted_iota(jnp.int32, shape, 0)
    eye = lane == sub
    eye_high = lane == sub + 64
    lane8 = lax.broadcasted_iota(jnp.int32, (8, 128), 1)
    sub8 = lax.broadcasted_iota(jnp.int32, (8, 128), 0)

    def lane_sum(values):
        return jnp.broadcast_to(jnp.sum(values, axis=1, keepdims=True), values.shape)

    def to_column(row, where=eye):
        return lane_sum(jnp.where(where, jnp.broadcast_to(row, shape), 0.0))

    def to_row(column, where=eye):
        return jnp.sum(jnp.where(where, column, 0.0), axis=0, keepdims=True)

    def project(read, count, kind, spans, fresh, square=False):
        every_one = count + square
        for first in range(0, every_one, 20):
            group = range(first, min(first + 20, every_one))

            def step(r, sums):
                at = pl.ds(pl.multiple_of(r * 8, 8), 8)
                other = read(at)
                return tuple(
                    acc + fold_lanes((vecs[i, at, :] if i < count else other) * other)
                    for i, acc in zip(group, sums)
                )

            if fresh:
                sums = (jnp.zeros((8, 128), jnp.float32),) * len(group)
            else:
                sums = tuple(proj[kind, i] for i in group)
            for start, length in spans:
                base = start // 8
                sums = lax.fori_loop(0, length // 8, lambda r, s: step(base + r, s), sums, unroll=4)
            for i, acc in zip(group, sums):
                proj[kind, i] = acc

    def project_late(step, count, p, halo, factor, h):
        square = step == STEPS - 1
        every_one = count + square
        for first in range(0, every_one, 20):
            group = range(first, min(first + 20, every_one))

            def add(r, sums):
                at = pl.ds(pl.multiple_of(p * rows_y + h * rows_half + r * 8, 8), 8)
                other = padded[step, halo, pl.ds(pl.multiple_of(8 + h * rows_half + r * 8, 8), 8), :] * factor
                whole = other
                if every_one in (group.stop,):
                    whole = image[at, :] + other
                    image[at, :] = whole
                return tuple(
                    acc + fold_lanes(vecs[i, at, :] * other if i < count else whole * whole)
                    for i, acc in zip(group, sums)
                )

            sums = lax.fori_loop(0, rows_half // 8, add, tuple(proj[0, i] for i in group), unroll=True)
            for i, acc in zip(group, sums):
                proj[0, i] = acc

    def projected(kind):
        return lane_sum(jnp.sum(proj[kind], axis=1))

    def stencil(step, part):
        tall = 16
        lanes = lax.broadcasted_iota(jnp.int32, (tall, width), 1)
        sx, sy, sz = WIND_SPEEDS
        centre = 6.0 + 1.5 * (sx + sy + sz)

        def piece(p, q):
            base = pl.multiple_of(q * tall, 8)
            at = pl.ds(pl.multiple_of(base + 8, 8), tall)
            block = padded[step, p + 2, pl.ds(base, tall + 16), :]
            here = block[8 : tall + 8]
            out_at = pl.ds(pl.multiple_of(p * rows_y + base, 8), tall)
            total = -(react[out_at, :] + centre) * here
            total = total + padded[step, p + 3, at, :] if p < planes - 1 else total
            total = total + (1.0 + 2.0 * sx) * padded[step, p + 1, at, :]
            total = total - (0.5 * sx) * padded[step, p, at, :] if p > 0 else total
            total = total + roll(block, tall + 15, 0)[8 : tall + 8]
            total = total + (1.0 + 2.0 * sy) * roll(block, 1, 0)[8 : tall + 8]
            total = total - (0.5 * sy) * roll(block, 2, 0)[8 : tall + 8]
            total = total + jnp.where(lanes < width - 1, roll(here, width - 1, 1), 0.0)
            total = total + (1.0 + 2.0 * sz) * jnp.where(lanes >= 1, roll(here, 1, 1), 0.0)
            total = total - (0.5 * sz) * jnp.where(lanes >= 2, roll(here, 2, 1), 0.0)
            image[out_at, :] = total

        for p in part:
            @pl.loop(0, rows_y // tall, unroll=True)
            def _(q, p=p):
                piece(p, q)

    def widen(values):
        return jnp.concatenate([values] * (width // 128), axis=1)

    def combine(step, count, scale, inverse=None):
        scale_row = widen(scale)
        more = step < STEPS - 1

        def plane(p, start, tall):
            at = pl.ds(pl.multiple_of(p * rows_y + start, 8), tall)
            total = image[at, :] * scale_row
            for i in range(count):
                total = total - coef[i : i + 1, :] * vecs[i, at, :]
            if more:
                vecs[keep + step, at, :] = total
                padded[step + 1, p + 2, start + 8 : start + 8 + tall, :] = total
            else:
                w_out[step, at, :] = total * widen(inverse)
                if step > 0:
                    w_out[step - 1, at, :] = vecs[keep + step - 1, at, :] * scale_row

        for n, (p_even, p_odd, n_even, n_odd) in enumerate((
            (0, planes - 1, 4, 0),
            (planes - 1, planes - 2, 0, 2),
            (planes - 2, 0, 2, 4),
        )):
            p = jnp.where(even, p_even, p_odd)
            if n > 0:
                plane(p, 0, rows_y)
            for h in range(2):
                if n == 0:
                    plane(p, h * rows_half, rows_half)
                if more:
                    start_halo(step + 1, (n_even + h,), even)
                    start_halo(step + 1, (n_odd + h,), odd)
        for p in range(1, planes - 2):
            plane(p, 0, rows_y)
        if more:
            start_halo(step + 1, (6, 7))

    def outer(a, b):
        return lax.dot_general(
            a, b, (((1,), (1,)), ((), ())), preferred_element_type=jnp.float32
        )

    cut = head.shape[1]
    late = keep * 8 - 128

    def gram_block(r):
        at = pl.ds(pl.multiple_of(r, 8), 8)
        values = vecs[0:keep, at, :].reshape(keep * 8, width)
        power = values * values
        squares[...] = squares[...] + power[:, :128] + power[:, 128:]
        high = values.astype(jnp.bfloat16)
        low = (values - high.astype(jnp.float32)).astype(jnp.bfloat16)
        left = jnp.concatenate([high[:cut] * 0.5, high[cut:]], axis=0)
        first = outer(left, high[:cut]) + outer(low, high[:cut])
        second = outer(low, high[late:])
        third = outer(high[cut:] * 0.5, high[late:])
        return first, second, third

    @pl.loop(0, chunks)
    def _(c):
        @pl.when(c == 1)
        def _():
            pl.semaphore_wait(barrier, expected)
            for d in range(1, n2):
                pl.semaphore_signal(ready, inc=1, device_id=member2(d)[1], device_id_type=MESH)
            pltpu.make_async_copy(all_last, all_last, last_sem).wait()
            start_halo(0, (4, 5, 0, 1, 2, 3), even)
            start_halo(0, (0, 1, 2, 3, 4, 5), odd)
            start_halo(0, (6, 7))

        load(c).wait()
        found = [gram_block(c * CHUNK + s) for s in range(0, CHUNK, 8)]
        first, second, third = (functools.reduce(lambda a, b: a + b, f) for f in zip(*found))
        head[...] = head[...] + first
        tail[...] = tail[...] + second
        tail[cut:, :] = tail[cut:, :] + third

    def picked(values, start):
        row = lax.broadcasted_iota(jnp.int32, values.shape, 0)
        column = lax.broadcasted_iota(jnp.int32, values.shape, 1)
        use = (lax.rem(row, 8) == lax.rem(column, 8)) & (column + start >= (cut if start else 0))
        kept = jnp.where(use, values, 0.0)
        return jnp.sum(kept.reshape(keep, 8, values.shape[1]), axis=1)

    spread = jnp.concatenate([picked(head[...], 0), picked(tail[...], late)], axis=1)
    place = lax.broadcasted_iota(jnp.int32, (cut + 128, 128), 0)
    place = jnp.where(place < cut, place, place - cut + late) // 8
    choose = jnp.where(place == lax.broadcasted_iota(jnp.int32, place.shape, 1), 1.0, 0.0)
    choose = choose.astype(jnp.bfloat16)
    half = jnp.zeros((keep, 128), jnp.float32)
    for _ in range(3):
        term = spread.astype(jnp.bfloat16)
        spread = spread - term.astype(jnp.float32)
        half = half + jnp.dot(term, choose, preferred_element_type=jnp.float32)
    diagonal = jnp.sum(jnp.sum(squares[...].reshape(keep, 8, 128), axis=1), axis=1, keepdims=True)
    lane_k = lax.broadcasted_iota(jnp.int32, (keep, 128), 1)
    sub_k = lax.broadcasted_iota(jnp.int32, (keep, 128), 0)
    image[0:128, 0:128] = jnp.zeros((128, 128), jnp.float32)
    image[0:keep, 0:128] = half
    turned = jnp.transpose(image[0:128, 0:128])
    pack[...] = jnp.zeros(pack.shape, jnp.float32)
    pack[0:keep] = jnp.where(lane_k == sub_k, diagonal, half + turned[0:keep])
    band = slots1.shape[1]
    folded = jnp.zeros((band, 128), jnp.float32)
    bands = [(g, g * band, min(g * band + band, padded_count)) for g in range(-(-padded_count // band))]
    for g, start, stop in bands:
        part = pack[start:stop]
        if stop - start < band:
            part = jnp.concatenate([part, jnp.zeros((band - stop + start, 128), jnp.float32)], axis=0)
        folded = folded + (roll(part, g * padded_count, 1) if g else part)
    slots1[me1] = folded

    def unfold(values):
        parts = [
            (roll(values, 128 - g * padded_count, 1) if g else values)[0 : stop - start]
            for g, start, stop in bands
        ]
        return jnp.where(lane < padded_count, jnp.concatenate(parts, axis=0), 0.0)

    def finish_gram():
        total, rest = exact_tree(exchange(stage2, False))
        row = lax.broadcasted_iota(jnp.int32, total.shape, 0)
        column = lax.broadcasted_iota(jnp.int32, total.shape, 1)
        ones = jnp.zeros(total.shape, jnp.float32)
        for g, start, _ in bands:
            on = (column == row + start + g * padded_count) & (row + start < keep)
            ones = jnp.where(on, cells, ones)
        return unfold(((ones - total) - rest) / cells)

    react_copy.wait()
    exchange(stage1, True)

    everything = [(0, rows)]

    def span(p, n=1):
        return [(p * rows_y, n * rows_y)]

    def project_image(step, spans, fresh=False, square=False):
        project(lambda at: image[at, :], keep + step, 0, spans, fresh, square)

    sx = WIND_SPEEDS[0]
    order = (
        [(0, 0, -0.5 * sx, h, 2 + h) for h in range(2)],
        [(planes - 1, planes + 2, 1.0, h, 4 + h) for h in range(2)],
    )

    def emit(step, scale):
        scale_row = widen(scale)

        @pl.loop(0, rows // 32)
        def _(q):
            at = pl.ds(pl.multiple_of(q * 32, 32), 32)
            w_out[step, at, :] = vecs[keep + step, at, :] * scale_row

    gap = None
    scales = jnp.ones(shape, jnp.float32)
    scales_row = jnp.ones((1, 128), jnp.float32)
    lane1 = lax.broadcasted_iota(jnp.int32, (1, 128), 1)
    hess = jnp.zeros((8, 128), jnp.float32)
    b_row = jnp.zeros((1, 128), jnp.float32)
    scale = jnp.ones((1, 128), jnp.float32)
    inverse = None
    for step in range(STEPS):
        count = keep + step
        last = count - 1
        if step > 0:
            project(lambda at: vecs[last, at, :], count, 1, everything, True)
            b_row = to_row(projected(1), eye_high)
        square = step == STEPS - 1
        wait_halo(step, (6, 7))
        stencil(step, range(2, planes))
        project_image(step, span(2, planes - 3), True, square)
        project_image(step, span(planes - 1))
        if step > 1:
            emit(step - 2, scale)
        wait_halo(step, (0, 1))
        stencil(step, range(2))
        project_image(step, span(0))
        project_image(step, span(1), False, square)
        for first, second in zip(order[0] + order[1], order[1] + order[0]):
            wait_halo(step, (first[4],), even)
            wait_halo(step, (second[4],), odd)
            p, halo, factor = (jnp.where(even, a, b) for a, b in zip(first[:3], second[:3]))
            project_late(step, count, p, halo, factor, first[3])
        row = to_row(projected(0)) + b_row
        if step == 0:
            pl.semaphore_wait(ready, n2 - 1)
        begin_sum(step, row)
        drain_halo(step)
        if step == 0:
            slots2[me2] = tree(exchange(stage1, False))
            exchange(stage2, True)
            gap = finish_gram()
            total, rest = finish_sum(0)
        else:
            total, rest = finish_sum(step)
            overlap = to_column(total, eye_high)
            length = overlap[last : last + 1]
            length_rest = lane_sum(jnp.where(lane1 == 64 + last, rest, 0.0))
            norm = jnp.sqrt(length + EPSILON)
            scale = 1.0 / norm
            hess = jnp.where((sub8 == step - 1) & (lane8 == last), norm, hess)
            scales = jnp.where(sub == last, scale, scales)
            scales_row = jnp.where(lane1 == last, scale, scales_row)
            square, square_rest = two_product(scale, scale)
            unit, unit_rest = two_product(length, square)
            own = (((1.0 - unit) - unit_rest) - length * square_rest) - length_rest * square
            column = jnp.where(sub < last, -overlap * scales * scale, 0.0)
            column = jnp.where(sub == last, own, column)
            gap = jnp.where(sub == last, to_row(column), gap)
            gap = jnp.where(lane == last, column, gap)
        first = jnp.where(sub < count, to_column(total) * scales * scale, 0.0)
        second = lane_sum(gap * to_row(first))
        weights = jnp.where(sub < count, first + second, 0.0)
        scaled = weights * scales
        coef[...] = widen(scaled)
        if step == STEPS - 1:
            parts, parts_rest = two_product(total, scales_row)
            parts_rest = parts_rest + rest * scales_row
            power, power_rest = two_product(parts, parts)
            power_rest = power_rest + 2.0 * parts * parts_rest
            whole = jnp.where(lane1 == count, total, 0.0)
            power = jnp.where(lane1 < count, power, -whole)
            power_rest = jnp.where(lane1 < count, power_rest, jnp.where(lane1 == count, -rest, 0.0))
            grid = lane_sum(whole) * 128.0
            coarse = (power + grid) - grid
            left = -(lane_sum(coarse) + lane_sum((power - coarse) + power_rest))
            third = lane_sum(gap * to_row(second))
            left = left * scale * scale - jnp.sum(first * second + weights * third, axis=0, keepdims=True)
            norm = jnp.sqrt(jnp.maximum(left, 0.0) + EPSILON)
            inverse = 1.0 / norm
            hess = jnp.where((sub8 == step) & (lane8 == count), norm, hess)
        hess = jnp.where((sub8 == step) & (lane8 < count), to_row(weights), hess)
        if step == STEPS - 1:
            h_out[...] = hess
        combine(step, count, scale, inverse)


def group_of(count):
    for size in (4, 2):
        if count % size == 0:
            return size
    return 1


def body(basis_vectors, reaction):
    keep, planes, rows_y, width = basis_vectors.shape
    n_gx, n_gy = lax.axis_size("gx"), lax.axis_size("gy")
    g1 = group_of(n_gx)
    n1, n2 = g1 * n_gy, n_gx // g1
    size = keep + STEPS
    padded_count = -(-size // 8) * 8
    rows = planes * rows_y
    rounds = STEPS
    band = -(-padded_count // (128 // padded_count) // 8) * 8
    f32 = jnp.float32
    dma = pltpu.SemaphoreType.DMA
    held = [
        pltpu.with_memory_space_constraint(x, pltpu.HBM)
        for x in (basis_vectors.reshape(keep, rows, width), reaction.reshape(rows, width))
    ]
    w, h = pl.pallas_call(
        functools.partial(kernel, keep, planes, rows_y, n_gx, n_gy, g1),
        out_shape=(
            jax.ShapeDtypeStruct((STEPS, rows, width), f32),
            jax.ShapeDtypeStruct((8, 128), f32),
        ),
        in_specs=[pl.BlockSpec(memory_space=pltpu.HBM)] * 2,
        out_specs=(pl.BlockSpec(memory_space=pltpu.VMEM),) * 2,
        scratch_shapes=[
            pltpu.VMEM((size, rows, width), f32),
            pltpu.VMEM((STEPS, planes + 3, rows_y + 16, width), f32),
            pltpu.VMEM((rows, width), f32),
            pltpu.VMEM((rows, width), f32),
            pltpu.VMEM((keep * 8, 256), f32),
            pltpu.VMEM((keep * 8, 128), f32),
            pltpu.VMEM((keep * 8, 128), f32),
            pltpu.VMEM((padded_count, 128), f32),
            pltpu.VMEM((2, padded_count, 8, 128), f32),
            pltpu.VMEM((n1, band, 128), f32),
            pltpu.VMEM((n2, band, 128), f32),
            pltpu.VMEM((rounds, n_gx * n_gy, 1, 128), f32),
            pltpu.VMEM((padded_count, width), f32),
            dma((rows // CHUNK,)),
            dma,
            dma,
            dma((4,)),
            dma((8,)),
            dma,
            dma,
            dma,
            dma,
            dma,
            dma((2,)),
            pltpu.SemaphoreType.REGULAR,
        ],
        compiler_params=pltpu.CompilerParams(
            collective_id=0, has_side_effects=True, vmem_limit_bytes=48 * 1024 * 1024
        ),
    )(*held)
    return w.reshape(STEPS, planes, rows_y, width), h[:STEPS, :size].T


def solution(mesh):
    in_specs = (P(None, "gx", "gy", None), P("gx", "gy", None))
    out_specs = (P(None, "gx", "gy", None), P())
    return jax.shard_map(body, mesh=mesh, in_specs=in_specs, out_specs=out_specs, check_vma=False)
```

```python
import functools

import jax
import jax.numpy as jnp
from jax import lax
from jax.experimental import pallas as pl
from jax.experimental.pallas import tpu as pltpu
from jax.sharding import PartitionSpec as P

STEPS = 4
WIND_SPEEDS = (0.9, 0.6, 0.4)
EPSILON = 1e-06
MESH = pl.DeviceIdType.MESH
CHUNK = 32


def roll(values, shift, axis):
    return pltpu.roll(values, shift, axis)


def fold_lanes(values):
    parts = [values[:, s : s + 128] for s in range(0, values.shape[1], 128)]
    return functools.reduce(lambda a, b: a + b, parts)


def two_sum(a, b):
    total = a + b
    other = total - a
    return total, (a - (total - other)) + (b - other)


def halves(a):
    scaled = a * 4097.0
    high = scaled - (scaled - a)
    return high, a - high


def two_product(a, b):
    product = a * b
    ah, al = halves(a)
    bh, bl = halves(b)
    return product, ((ah * bh - product) + ah * bl + al * bh) + al * bl


def exact_tree(parts):
    def add(a, b):
        total, rest = two_sum(a[0], b[0])
        return total, (a[1] + b[1]) + rest

    pairs = [(part, jnp.zeros_like(part)) for part in parts]
    while len(pairs) > 1:
        pairs = [
            add(pairs[i], pairs[i + 1]) if i + 1 < len(pairs) else pairs[i]
            for i in range(0, len(pairs), 2)
        ]
    return pairs[0]


def kernel(
    keep, planes, rows_y, n_gx, n_gy, g1,
    basis, reaction, w_out, h_out,
    vecs, padded, image, react, head, tail, squares, pack, proj, grams, slots, coef,
    load_sem, last_sem, react_sem,
    halo_send, halo_recv, gram_send, gram_recv, sends, recvs, ready,
):
    width = basis.shape[2]
    rows = planes * rows_y
    padded_count = proj.shape[1]
    gx = lax.axis_index("gx")
    gy = lax.axis_index("gy")
    n1 = n_gy * g1
    n2 = n_gx // g1
    low = lax.rem(gx, g1)
    high = gx // g1
    me1 = gy * g1 + low
    me2 = high
    cells = float(rows * width * n_gx * n_gy)

    last_copies = [
        pltpu.make_async_copy(
            basis.at[keep - 1, p * rows_y : (p + 1) * rows_y],
            padded.at[0, p + 2, 8 : rows_y + 8],
            last_sem,
        )
        for p in range(planes)
    ]
    for copy in last_copies:
        copy.start()
    all_last = padded.at[0, 2 : planes + 2, 8 : rows_y + 8]
    chunks = rows // CHUNK

    def load(c):
        at = pl.ds(pl.multiple_of(c * CHUNK, CHUNK), CHUNK)
        return pltpu.make_async_copy(basis.at[:, at], vecs.at[0:keep, at], load_sem.at[c])

    @pl.loop(0, chunks)
    def _(c):
        load(c).start()

    react_copy = pltpu.make_async_copy(reaction, react, react_sem)
    react_copy.start()

    has_xl, has_xh = gx > 0, gx < n_gx - 1
    has_yl, has_yh = gy > 0, gy < n_gy - 1

    def member1(d):
        p = lax.rem(me1 + d, n1)
        return p, {"gx": high * g1 + lax.rem(p, g1), "gy": p // g1}

    def member2(d):
        p = lax.rem(me2 + d, n2)
        return p, {"gx": p * g1 + low, "gy": gy}

    me = gx * n_gy + gy
    devices = n_gx * n_gy

    bits = devices.bit_length() - 1
    turns = [(1 - 2 * lax.rem(me // 2**i, 2)) * 2**i for i in range(bits)]

    def member(d):
        if devices == 2**bits:
            p = me + functools.reduce(lambda a, b: a + b, [t for i, t in enumerate(turns) if d >> i & 1])
        else:
            p = lax.rem(me + d, devices)
        return {"gx": p // n_gy, "gy": lax.rem(p, n_gy)}

    barrier = pltpu.get_barrier_semaphore()
    for d in range(1, n1):
        pl.semaphore_signal(barrier, inc=1, device_id=member1(d)[1], device_id_type=MESH)
    for d in range(1, n2):
        pl.semaphore_signal(barrier, inc=1, device_id=member2(d)[1], device_id_type=MESH)
    sides = (
        (has_xh, {"gx": gx + 1, "gy": gy}),
        (has_xl, {"gx": gx - 1, "gy": gy}),
        (has_yh, {"gx": gx, "gy": gy + 1}),
        (has_yl, {"gx": gx, "gy": gy - 1}),
    )
    even = lax.rem(gx, 2) == 0
    odd = jnp.logical_not(even)
    expected = n1 - 1 + n2 - 1
    for there, device in sides:
        @pl.when(there)
        def _(device=device):
            pl.semaphore_signal(barrier, inc=1, device_id=device, device_id_type=MESH)

        expected = expected + there.astype(jnp.int32)

    zero_plane = jnp.zeros((1, rows_y, width), jnp.float32)
    zero_rows = jnp.zeros((planes, 8, width), jnp.float32)
    for step in range(STEPS):
        @pl.when(jnp.logical_not(has_xl))
        def _(step=step):
            padded[step, 0:1, 8 : rows_y + 8] = zero_plane
            padded[step, 1:2, 8 : rows_y + 8] = zero_plane

        @pl.when(jnp.logical_not(has_xh))
        def _(step=step):
            padded[step, planes + 2 : planes + 3, 8 : rows_y + 8] = zero_plane

        @pl.when(jnp.logical_not(has_yl))
        def _(step=step):
            padded[step, 2 : planes + 2, 0:8] = zero_rows

        @pl.when(jnp.logical_not(has_yh))
        def _(step=step):
            padded[step, 2 : planes + 2, rows_y + 8 : rows_y + 16] = zero_rows

    head[...] = jnp.zeros(head.shape, jnp.float32)
    tail[...] = jnp.zeros(tail.shape, jnp.float32)
    squares[...] = jnp.zeros(squares.shape, jnp.float32)
    proj[...] = jnp.zeros(proj.shape, jnp.float32)
    rows_half = rows_y // 2

    def halo_copies(step):
        own = pl.ds(2, planes)
        part = [slice(8 + h * rows_half, 8 + (h + 1) * rows_half) for h in range(2)]
        refs = [
            (side, padded.at[step, src, at], padded.at[step, dst, at])
            for side, src, dst in ((0, planes + 1, 1), (0, planes, 0), (1, 2, planes + 2))
            for at in part
        ] + [
            (2, padded.at[step, own, rows_y : rows_y + 8], padded.at[step, own, 0:8]),
            (3, padded.at[step, own, 8:16], padded.at[step, own, rows_y + 8 : rows_y + 16]),
        ]
        return [
            (
                sides[side][0],
                (has_xl, has_xh, has_yl, has_yh)[side],
                pltpu.make_async_remote_copy(
                    src_ref=src, dst_ref=dst,
                    send_sem=halo_send.at[side], recv_sem=halo_recv.at[n],
                    device_id=sides[side][1], device_id_type=MESH,
                ),
            )
            for n, (side, src, dst) in enumerate(refs)
        ]

    def start_halo(step, which, where=None):
        copies = halo_copies(step)
        for n in which:
            there, _, copy = copies[n]

            @pl.when(there if where is None else there & where)
            def _(copy=copy):
                copy.start()

    def wait_halo(step, which, where=None):
        copies = halo_copies(step)
        for n in which:
            _, arrives, copy = copies[n]

            @pl.when(arrives if where is None else arrives & where)
            def _(copy=copy):
                copy.wait_recv()

    def drain_halo(step):
        inside = slice(8, rows_y + 8)
        copies = halo_copies(step)
        groups = (
            padded.at[step, planes : planes + 2, inside],
            padded.at[step, 2:3, inside],
        )
        for side, group in enumerate(groups):
            @pl.when(sides[side][0])
            def _(side=side, group=group):
                pltpu.make_async_remote_copy(
                    src_ref=group, dst_ref=group,
                    send_sem=halo_send.at[side], recv_sem=halo_recv.at[0],
                    device_id=sides[side][1], device_id_type=MESH,
                ).wait_send()

        for there, _, copy in copies[6:]:
            @pl.when(there)
            def _(copy=copy):
                copy.wait_send()

    def gram_copy(at, d):
        return pltpu.make_async_remote_copy(
            src_ref=grams.at[at], dst_ref=grams.at[at], send_sem=gram_send, recv_sem=gram_recv,
            device_id=member(d), device_id_type=MESH,
        )

    def begin_sum(rnd, row):
        slots[rnd, me] = row
        for d in range(devices - 1, 0, -1):
            pltpu.make_async_remote_copy(
                src_ref=slots.at[rnd, me], dst_ref=slots.at[rnd, me],
                send_sem=sends, recv_sem=recvs.at[rnd % 2],
                device_id=member(d), device_id_type=MESH,
            ).start()

    def every(rnd):
        return pltpu.make_async_remote_copy(
            src_ref=slots.at[rnd, 0 : devices - 1], dst_ref=slots.at[rnd, 0 : devices - 1],
            send_sem=sends, recv_sem=recvs.at[rnd % 2],
            device_id=member(1), device_id_type=MESH,
        )

    def finish_sum(rnd):
        every(rnd).wait_recv()
        every(rnd).wait_send()
        total, rest = exact_tree([slots[rnd, slot] for slot in range(devices)])
        return total / cells, rest / cells

    shape = (padded_count, 128)
    lane = lax.broadcasted_iota(jnp.int32, shape, 1)
    sub = lax.broadcasted_iota(jnp.int32, shape, 0)
    eye = lane == sub
    eye_high = lane == sub + 64
    lane8 = lax.broadcasted_iota(jnp.int32, (8, 128), 1)
    sub8 = lax.broadcasted_iota(jnp.int32, (8, 128), 0)

    def lane_sum(values):
        return jnp.broadcast_to(jnp.sum(values, axis=1, keepdims=True), values.shape)

    def to_column(row, where=eye):
        return lane_sum(jnp.where(where, jnp.broadcast_to(row, shape), 0.0))

    def to_row(column, where=eye):
        return jnp.sum(jnp.where(where, column, 0.0), axis=0, keepdims=True)

    def project(read, count, kind, spans, fresh, square=False):
        every_one = count + square
        for first in range(0, every_one, 20):
            group = range(first, min(first + 20, every_one))

            def step(r, sums):
                at = pl.ds(pl.multiple_of(r * 8, 8), 8)
                other = read(at)
                return tuple(
                    acc + fold_lanes((vecs[i, at, :] if i < count else other) * other)
                    for i, acc in zip(group, sums)
                )

            if fresh:
                sums = (jnp.zeros((8, 128), jnp.float32),) * len(group)
            else:
                sums = tuple(proj[kind, i] for i in group)
            for start, length in spans:
                base = start // 8
                sums = lax.fori_loop(0, length // 8, lambda r, s: step(base + r, s), sums, unroll=4)
            for i, acc in zip(group, sums):
                proj[kind, i] = acc

    def project_late(step, count, p, halo, factor, h):
        square = step == STEPS - 1
        every_one = count + square
        for first in range(0, every_one, 20):
            group = range(first, min(first + 20, every_one))

            def add(r, sums):
                at = pl.ds(pl.multiple_of(p * rows_y + h * rows_half + r * 8, 8), 8)
                other = padded[step, halo, pl.ds(pl.multiple_of(8 + h * rows_half + r * 8, 8), 8), :] * factor
                whole = other
                if every_one in (group.stop,):
                    whole = image[at, :] + other
                    image[at, :] = whole
                return tuple(
                    acc + fold_lanes(vecs[i, at, :] * other if i < count else whole * whole)
                    for i, acc in zip(group, sums)
                )

            sums = lax.fori_loop(0, rows_half // 8, add, tuple(proj[0, i] for i in group), unroll=True)
            for i, acc in zip(group, sums):
                proj[0, i] = acc

    def projected(kind):
        return lane_sum(jnp.sum(proj[kind], axis=1))

    def stencil(step, part):
        tall = 16
        lanes = lax.broadcasted_iota(jnp.int32, (tall, width), 1)
        sx, sy, sz = WIND_SPEEDS
        centre = 6.0 + 1.5 * (sx + sy + sz)

        def piece(p, q):
            base = pl.multiple_of(q * tall, 8)
            at = pl.ds(pl.multiple_of(base + 8, 8), tall)
            block = padded[step, p + 2, pl.ds(base, tall + 16), :]
            here = block[8 : tall + 8]
            out_at = pl.ds(pl.multiple_of(p * rows_y + base, 8), tall)
            total = -(react[out_at, :] + centre) * here
            total = total + padded[step, p + 3, at, :] if p < planes - 1 else total
            total = total + (1.0 + 2.0 * sx) * padded[step, p + 1, at, :]
            total = total - (0.5 * sx) * padded[step, p, at, :] if p > 0 else total
            total = total + roll(block, tall + 15, 0)[8 : tall + 8]
            total = total + (1.0 + 2.0 * sy) * roll(block, 1, 0)[8 : tall + 8]
            total = total - (0.5 * sy) * roll(block, 2, 0)[8 : tall + 8]
            total = total + jnp.where(lanes < width - 1, roll(here, width - 1, 1), 0.0)
            total = total + (1.0 + 2.0 * sz) * jnp.where(lanes >= 1, roll(here, 1, 1), 0.0)
            total = total - (0.5 * sz) * jnp.where(lanes >= 2, roll(here, 2, 1), 0.0)
            image[out_at, :] = total

        for p in part:
            @pl.loop(0, rows_y // tall, unroll=True)
            def _(q, p=p):
                piece(p, q)

    def widen(values):
        return jnp.concatenate([values] * (width // 128), axis=1)

    def combine(step, count, scale, inverse=None):
        scale_row = widen(scale)
        more = step < STEPS - 1

        def plane(p, start, tall):
            at = pl.ds(pl.multiple_of(p * rows_y + start, 8), tall)
            total = image[at, :] * scale_row
            for i in range(count):
                total = total - coef[i : i + 1, :] * vecs[i, at, :]
            if more:
                vecs[keep + step, at, :] = total
                padded[step + 1, p + 2, start + 8 : start + 8 + tall, :] = total
            else:
                w_out[step, at, :] = total * widen(inverse)
                if step > 0:
                    w_out[step - 1, at, :] = vecs[keep + step - 1, at, :] * scale_row

        for n, (p_even, p_odd, n_even, n_odd) in enumerate((
            (0, planes - 1, 4, 0),
            (planes - 1, planes - 2, 0, 2),
            (planes - 2, 0, 2, 4),
        )):
            p = jnp.where(even, p_even, p_odd)
            if n > 0:
                plane(p, 0, rows_y)
            for h in range(2):
                if n == 0:
                    plane(p, h * rows_half, rows_half)
                if more:
                    start_halo(step + 1, (n_even + h,), even)
                    start_halo(step + 1, (n_odd + h,), odd)
        for p in range(1, planes - 2):
            plane(p, 0, rows_y)
        if more:
            start_halo(step + 1, (6, 7))

    def outer(a, b):
        return lax.dot_general(
            a, b, (((1,), (1,)), ((), ())), preferred_element_type=jnp.float32
        )

    cut = head.shape[1]
    late = keep * 8 - 128

    def gram_block(r):
        at = pl.ds(pl.multiple_of(r, 8), 8)
        values = vecs[0:keep, at, :].reshape(keep * 8, width)
        power = values * values
        squares[...] = squares[...] + power[:, :128] + power[:, 128:]
        high = values.astype(jnp.bfloat16)
        low = (values - high.astype(jnp.float32)).astype(jnp.bfloat16)
        left = jnp.concatenate([high[:cut] * 0.5, high[cut:]], axis=0)
        first = outer(left, high[:cut]) + outer(low, high[:cut])
        second = outer(low, high[late:])
        third = outer(high[cut:] * 0.5, high[late:])
        return first, second, third

    @pl.loop(0, chunks)
    def _(c):
        @pl.when(c == 1)
        def _():
            pl.semaphore_wait(barrier, expected)
            for d in range(1, n2):
                pl.semaphore_signal(ready, inc=1, device_id=member2(d)[1], device_id_type=MESH)
            pltpu.make_async_copy(all_last, all_last, last_sem).wait()
            start_halo(0, (4, 5, 0, 1, 2, 3), even)
            start_halo(0, (0, 1, 2, 3, 4, 5), odd)
            start_halo(0, (6, 7))

        load(c).wait()
        found = [gram_block(c * CHUNK + s) for s in range(0, CHUNK, 8)]
        first, second, third = (functools.reduce(lambda a, b: a + b, f) for f in zip(*found))
        head[...] = head[...] + first
        tail[...] = tail[...] + second
        tail[cut:, :] = tail[cut:, :] + third

    def picked(values, start):
        row = lax.broadcasted_iota(jnp.int32, values.shape, 0)
        column = lax.broadcasted_iota(jnp.int32, values.shape, 1)
        use = (lax.rem(row, 8) == lax.rem(column, 8)) & (column + start >= (cut if start else 0))
        kept = jnp.where(use, values, 0.0)
        return jnp.sum(kept.reshape(keep, 8, values.shape[1]), axis=1)

    spread = jnp.concatenate([picked(head[...], 0), picked(tail[...], late)], axis=1)
    place = lax.broadcasted_iota(jnp.int32, (cut + 128, 128), 0)
    place = jnp.where(place < cut, place, place - cut + late) // 8
    choose = jnp.where(place == lax.broadcasted_iota(jnp.int32, place.shape, 1), 1.0, 0.0)
    choose = choose.astype(jnp.bfloat16)
    half = jnp.zeros((keep, 128), jnp.float32)
    for _ in range(3):
        term = spread.astype(jnp.bfloat16)
        spread = spread - term.astype(jnp.float32)
        half = half + jnp.dot(term, choose, preferred_element_type=jnp.float32)
    diagonal = jnp.sum(jnp.sum(squares[...].reshape(keep, 8, 128), axis=1), axis=1, keepdims=True)
    lane_k = lax.broadcasted_iota(jnp.int32, (keep, 128), 1)
    sub_k = lax.broadcasted_iota(jnp.int32, (keep, 128), 0)
    pack[...] = jnp.zeros(pack.shape, jnp.float32)
    pack[0:keep] = half
    turned = jnp.transpose(pack[...])
    pack[0:keep] = jnp.where(lane_k == sub_k, diagonal, half + turned[0:keep])
    blocks, start = [], 0
    for b in range(0, keep, 8):
        blocks.append((b, start))
        start += keep - b
    folded = jnp.zeros((8, 128), jnp.float32)
    for b, start in blocks:
        part = jnp.where((lane8 >= b) & (lane8 < keep), pack[b : b + 8], 0.0)
        folded = folded + (roll(part, start - b, 1) if start > b else part)
    grams[me] = folded
    pl.semaphore_wait(ready, n2 - 1)
    for d in range(devices - 1, 0, -1):
        gram_copy(me, d).start()

    def finish_gram():
        arrived = gram_copy(pl.ds(0, devices - 1), 1)
        arrived.wait_recv()
        arrived.wait_send()
        total, rest = exact_tree([grams[slot] for slot in range(devices)])
        ones = jnp.zeros((8, 128), jnp.float32)
        for b, start in blocks:
            ones = jnp.where((lane8 == sub8 + start) & (sub8 + b < keep), cells, ones)
        values = ((ones - total) - rest) / cells
        parts = []
        for b, start in blocks:
            part = roll(values, 128 + b - start, 1) if start > b else values
            parts.append(jnp.where((lane8 >= b) & (lane8 < keep), part, 0.0))
        upper = jnp.concatenate(parts, axis=0)
        pack[0 : 8 * len(parts)] = upper
        lower = jnp.transpose(pack[...])[0 : 8 * len(parts)]
        rows_of = lax.broadcasted_iota(jnp.int32, upper.shape, 0) // 8
        lanes_of = lax.broadcasted_iota(jnp.int32, upper.shape, 1) // 8
        return upper + jnp.where(rows_of > lanes_of, lower, 0.0)

    react_copy.wait()

    everything = [(0, rows)]

    def span(p, n=1):
        return [(p * rows_y, n * rows_y)]

    def project_image(step, spans, fresh=False, square=False):
        project(lambda at: image[at, :], keep + step, 0, spans, fresh, square)

    sx = WIND_SPEEDS[0]
    order = (
        [(0, 0, -0.5 * sx, h, 2 + h) for h in range(2)],
        [(planes - 1, planes + 2, 1.0, h, 4 + h) for h in range(2)],
    )

    def emit(step, scale):
        scale_row = widen(scale)

        @pl.loop(0, rows // 32)
        def _(q):
            at = pl.ds(pl.multiple_of(q * 32, 32), 32)
            w_out[step, at, :] = vecs[keep + step, at, :] * scale_row

    gap = None
    scales = jnp.ones(shape, jnp.float32)
    scales_row = jnp.ones((1, 128), jnp.float32)
    lane1 = lax.broadcasted_iota(jnp.int32, (1, 128), 1)
    hess = jnp.zeros((8, 128), jnp.float32)
    b_row = jnp.zeros((1, 128), jnp.float32)
    scale = jnp.ones((1, 128), jnp.float32)
    inverse = None
    for step in range(STEPS):
        count = keep + step
        last = count - 1
        if step > 0:
            project(lambda at: vecs[last, at, :], count, 1, everything, True)
            b_row = to_row(projected(1), eye_high)
        square = step == STEPS - 1
        wait_halo(step, (6, 7))
        stencil(step, range(2, planes))
        project_image(step, span(2, planes - 3), True, square)
        project_image(step, span(planes - 1))
        if step > 1:
            emit(step - 2, scale)
        wait_halo(step, (0, 1))
        stencil(step, range(2))
        project_image(step, span(0))
        project_image(step, span(1), False, square)
        for first, second in zip(order[0] + order[1], order[1] + order[0]):
            wait_halo(step, (first[4],), even)
            wait_halo(step, (second[4],), odd)
            p, halo, factor = (jnp.where(even, a, b) for a, b in zip(first[:3], second[:3]))
            project_late(step, count, p, halo, factor, first[3])
        row = to_row(projected(0)) + b_row
        begin_sum(step, row)
        drain_halo(step)
        if step == 0:
            gap = finish_gram()
            total, rest = finish_sum(0)
        else:
            total, rest = finish_sum(step)
            overlap = to_column(total, eye_high)
            length = overlap[last : last + 1]
            length_rest = lane_sum(jnp.where(lane1 == 64 + last, rest, 0.0))
            norm = jnp.sqrt(length + EPSILON)
            scale = 1.0 / norm
            hess = jnp.where((sub8 == step - 1) & (lane8 == last), norm, hess)
            scales = jnp.where(sub == last, scale, scales)
            scales_row = jnp.where(lane1 == last, scale, scales_row)
            square, square_rest = two_product(scale, scale)
            unit, unit_rest = two_product(length, square)
            own = (((1.0 - unit) - unit_rest) - length * square_rest) - length_rest * square
            column = jnp.where(sub < last, -overlap * scales * scale, 0.0)
            column = jnp.where(sub == last, own, column)
            gap = jnp.where(sub == last, to_row(column), gap)
            gap = jnp.where(lane == last, column, gap)
        first = jnp.where(sub < count, to_column(total) * scales * scale, 0.0)
        second = lane_sum(gap * to_row(first))
        weights = jnp.where(sub < count, first + second, 0.0)
        scaled = weights * scales
        coef[...] = widen(scaled)
        if step == STEPS - 1:
            parts, parts_rest = two_product(total, scales_row)
            parts_rest = parts_rest + rest * scales_row
            power, power_rest = two_product(parts, parts)
            power_rest = power_rest + 2.0 * parts * parts_rest
            whole = jnp.where(lane1 == count, total, 0.0)
            power = jnp.where(lane1 < count, power, -whole)
            power_rest = jnp.where(lane1 < count, power_rest, jnp.where(lane1 == count, -rest, 0.0))
            grid = lane_sum(whole) * 128.0
            coarse = (power + grid) - grid
            left = -(lane_sum(coarse) + lane_sum((power - coarse) + power_rest))
            third = lane_sum(gap * to_row(second))
            left = left * scale * scale - jnp.sum(first * second + weights * third, axis=0, keepdims=True)
            norm = jnp.sqrt(jnp.maximum(left, 0.0) + EPSILON)
            inverse = 1.0 / norm
            hess = jnp.where((sub8 == step) & (lane8 == count), norm, hess)
        hess = jnp.where((sub8 == step) & (lane8 < count), to_row(weights), hess)
        if step == STEPS - 1:
            h_out[...] = hess
        combine(step, count, scale, inverse)


def group_of(count):
    for size in (4, 2):
        if count % size == 0:
            return size
    return 1


def body(basis_vectors, reaction):
    keep, planes, rows_y, width = basis_vectors.shape
    n_gx, n_gy = lax.axis_size("gx"), lax.axis_size("gy")
    g1 = group_of(n_gx)
    size = keep + STEPS
    padded_count = -(-size // 8) * 8
    rows = planes * rows_y
    rounds = STEPS
    f32 = jnp.float32
    dma = pltpu.SemaphoreType.DMA
    held = [
        pltpu.with_memory_space_constraint(x, pltpu.HBM)
        for x in (basis_vectors.reshape(keep, rows, width), reaction.reshape(rows, width))
    ]
    w, h = pl.pallas_call(
        functools.partial(kernel, keep, planes, rows_y, n_gx, n_gy, g1),
        out_shape=(
            jax.ShapeDtypeStruct((STEPS, rows, width), f32),
            jax.ShapeDtypeStruct((8, 128), f32),
        ),
        in_specs=[pl.BlockSpec(memory_space=pltpu.HBM)] * 2,
        out_specs=(pl.BlockSpec(memory_space=pltpu.VMEM),) * 2,
        scratch_shapes=[
            pltpu.VMEM((size, rows, width), f32),
            pltpu.VMEM((STEPS, planes + 3, rows_y + 16, width), f32),
            pltpu.VMEM((rows, width), f32),
            pltpu.VMEM((rows, width), f32),
            pltpu.VMEM((keep * 8, 256), f32),
            pltpu.VMEM((keep * 8, 128), f32),
            pltpu.VMEM((keep * 8, 128), f32),
            pltpu.VMEM((128, 128), f32),
            pltpu.VMEM((2, padded_count, 8, 128), f32),
            pltpu.VMEM((n_gx * n_gy, 8, 128), f32),
            pltpu.VMEM((rounds, n_gx * n_gy, 1, 128), f32),
            pltpu.VMEM((padded_count, width), f32),
            dma((rows // CHUNK,)),
            dma,
            dma,
            dma((4,)),
            dma((8,)),
            dma,
            dma,
            dma,
            dma((2,)),
            pltpu.SemaphoreType.REGULAR,
        ],
        compiler_params=pltpu.CompilerParams(
            collective_id=0, has_side_effects=True, vmem_limit_bytes=48 * 1024 * 1024
        ),
    )(*held)
    return w.reshape(STEPS, planes, rows_y, width), h[:STEPS, :size].T


def solution(mesh):
    in_specs = (P(None, "gx", "gy", None), P("gx", "gy", None))
    out_specs = (P(None, "gx", "gy", None), P())
    return jax.shard_map(body, mesh=mesh, in_specs=in_specs, out_specs=out_specs, check_vma=False)
```

```python
import functools

import jax
import jax.numpy as jnp
from jax import lax
from jax.experimental import pallas as pl
from jax.experimental.pallas import tpu as pltpu
from jax.sharding import PartitionSpec as P

STEPS = 4
WIND_SPEEDS = (0.9, 0.6, 0.4)
EPSILON = 1e-06
MESH = pl.DeviceIdType.MESH
CHUNK = 32


def roll(values, shift, axis):
    return pltpu.roll(values, shift, axis)


def fold_lanes(values):
    parts = [values[:, s : s + 128] for s in range(0, values.shape[1], 128)]
    return functools.reduce(lambda a, b: a + b, parts)


def two_sum(a, b):
    total = a + b
    other = total - a
    return total, (a - (total - other)) + (b - other)


def halves(a):
    scaled = a * 4097.0
    high = scaled - (scaled - a)
    return high, a - high


def two_product(a, b):
    product = a * b
    ah, al = halves(a)
    bh, bl = halves(b)
    return product, ((ah * bh - product) + ah * bl + al * bh) + al * bl


def exact_tree(parts):
    def add(a, b):
        total, rest = two_sum(a[0], b[0])
        return total, (a[1] + b[1]) + rest

    pairs = [(part, jnp.zeros_like(part)) for part in parts]
    while len(pairs) > 1:
        pairs = [
            add(pairs[i], pairs[i + 1]) if i + 1 < len(pairs) else pairs[i]
            for i in range(0, len(pairs), 2)
        ]
    return pairs[0]


def kernel(
    keep, planes, rows_y, n_gx, n_gy, g1,
    basis, reaction, w_out, h_out,
    vecs, padded, image, react, head, tail, squares, pack, proj, grams, slots, coef,
    load_sem, last_sem, react_sem,
    halo_send, halo_recv, gram_send, gram_recv, sends, recvs, ready,
):
    width = basis.shape[2]
    rows = planes * rows_y
    padded_count = proj.shape[1]
    gx = lax.axis_index("gx")
    gy = lax.axis_index("gy")
    n1 = n_gy * g1
    n2 = n_gx // g1
    low = lax.rem(gx, g1)
    high = gx // g1
    me1 = gy * g1 + low
    me2 = high
    cells = float(rows * width * n_gx * n_gy)

    last_copies = [
        pltpu.make_async_copy(
            basis.at[keep - 1, p * rows_y : (p + 1) * rows_y],
            padded.at[0, p + 2, 8 : rows_y + 8],
            last_sem,
        )
        for p in range(planes)
    ]
    all_last = padded.at[0, 2 : planes + 2, 8 : rows_y + 8]
    chunks = rows // CHUNK

    def load(c):
        at = pl.ds(pl.multiple_of(c * CHUNK, CHUNK), CHUNK)
        return pltpu.make_async_copy(basis.at[:, at], vecs.at[0:keep, at], load_sem.at[c])

    load(0).start()
    for copy in last_copies:
        copy.start()

    @pl.loop(1, chunks)
    def _(c):
        load(c).start()

    react_copy = pltpu.make_async_copy(reaction, react, react_sem)
    react_copy.start()

    has_xl, has_xh = gx > 0, gx < n_gx - 1
    has_yl, has_yh = gy > 0, gy < n_gy - 1

    def member1(d):
        p = lax.rem(me1 + d, n1)
        return p, {"gx": high * g1 + lax.rem(p, g1), "gy": p // g1}

    def member2(d):
        p = lax.rem(me2 + d, n2)
        return p, {"gx": p * g1 + low, "gy": gy}

    me = gx * n_gy + gy
    devices = n_gx * n_gy

    bits = devices.bit_length() - 1
    turns = [(1 - 2 * lax.rem(me // 2**i, 2)) * 2**i for i in range(bits)]

    def member(d):
        if devices == 2**bits:
            p = me + functools.reduce(lambda a, b: a + b, [t for i, t in enumerate(turns) if d >> i & 1])
        else:
            p = lax.rem(me + d, devices)
        return {"gx": p // n_gy, "gy": lax.rem(p, n_gy)}

    barrier = pltpu.get_barrier_semaphore()
    for d in range(1, n1):
        pl.semaphore_signal(barrier, inc=1, device_id=member1(d)[1], device_id_type=MESH)
    for d in range(1, n2):
        pl.semaphore_signal(barrier, inc=1, device_id=member2(d)[1], device_id_type=MESH)
    sides = (
        (has_xh, {"gx": gx + 1, "gy": gy}),
        (has_xl, {"gx": gx - 1, "gy": gy}),
        (has_yh, {"gx": gx, "gy": gy + 1}),
        (has_yl, {"gx": gx, "gy": gy - 1}),
    )
    even = lax.rem(gx, 2) == 0
    odd = jnp.logical_not(even)
    expected = n1 - 1 + n2 - 1
    for there, device in sides:
        @pl.when(there)
        def _(device=device):
            pl.semaphore_signal(barrier, inc=1, device_id=device, device_id_type=MESH)

        expected = expected + there.astype(jnp.int32)

    zero_plane = jnp.zeros((1, rows_y, width), jnp.float32)
    zero_rows = jnp.zeros((planes, 8, width), jnp.float32)
    for step in range(STEPS):
        @pl.when(jnp.logical_not(has_xl))
        def _(step=step):
            padded[step, 0:1, 8 : rows_y + 8] = zero_plane
            padded[step, 1:2, 8 : rows_y + 8] = zero_plane

        @pl.when(jnp.logical_not(has_xh))
        def _(step=step):
            padded[step, planes + 2 : planes + 3, 8 : rows_y + 8] = zero_plane

        @pl.when(jnp.logical_not(has_yl))
        def _(step=step):
            padded[step, 2 : planes + 2, 0:8] = zero_rows

        @pl.when(jnp.logical_not(has_yh))
        def _(step=step):
            padded[step, 2 : planes + 2, rows_y + 8 : rows_y + 16] = zero_rows

    head[...] = jnp.zeros(head.shape, jnp.float32)
    tail[...] = jnp.zeros(tail.shape, jnp.float32)
    squares[...] = jnp.zeros(squares.shape, jnp.float32)
    proj[...] = jnp.zeros(proj.shape, jnp.float32)
    rows_half = rows_y // 2

    def halo_copies(step):
        own = pl.ds(2, planes)
        part = [slice(8 + h * rows_half, 8 + (h + 1) * rows_half) for h in range(2)]
        refs = [
            (side, padded.at[step, src, at], padded.at[step, dst, at])
            for side, src, dst in ((0, planes + 1, 1), (0, planes, 0), (1, 2, planes + 2))
            for at in part
        ] + [
            (2, padded.at[step, own, rows_y : rows_y + 8], padded.at[step, own, 0:8]),
            (3, padded.at[step, own, 8:16], padded.at[step, own, rows_y + 8 : rows_y + 16]),
        ]
        return [
            (
                sides[side][0],
                (has_xl, has_xh, has_yl, has_yh)[side],
                pltpu.make_async_remote_copy(
                    src_ref=src, dst_ref=dst,
                    send_sem=halo_send.at[side], recv_sem=halo_recv.at[n],
                    device_id=sides[side][1], device_id_type=MESH,
                ),
            )
            for n, (side, src, dst) in enumerate(refs)
        ]

    def start_halo(step, which, where=None):
        copies = halo_copies(step)
        for n in which:
            there, _, copy = copies[n]

            @pl.when(there if where is None else there & where)
            def _(copy=copy):
                copy.start()

    def wait_halo(step, which, where=None):
        copies = halo_copies(step)
        for n in which:
            _, arrives, copy = copies[n]

            @pl.when(arrives if where is None else arrives & where)
            def _(copy=copy):
                copy.wait_recv()

    def drain_halo(step):
        inside = slice(8, rows_y + 8)
        copies = halo_copies(step)
        groups = (
            padded.at[step, planes : planes + 2, inside],
            padded.at[step, 2:3, inside],
        )
        for side, group in enumerate(groups):
            @pl.when(sides[side][0])
            def _(side=side, group=group):
                pltpu.make_async_remote_copy(
                    src_ref=group, dst_ref=group,
                    send_sem=halo_send.at[side], recv_sem=halo_recv.at[0],
                    device_id=sides[side][1], device_id_type=MESH,
                ).wait_send()

        for there, _, copy in copies[6:]:
            @pl.when(there)
            def _(copy=copy):
                copy.wait_send()

    def gram_copy(at, d):
        return pltpu.make_async_remote_copy(
            src_ref=grams.at[at], dst_ref=grams.at[at], send_sem=gram_send, recv_sem=gram_recv,
            device_id=member(d), device_id_type=MESH,
        )

    def begin_sum(rnd, row):
        slots[rnd, me] = row
        for d in range(devices - 1, 0, -1):
            pltpu.make_async_remote_copy(
                src_ref=slots.at[rnd, me], dst_ref=slots.at[rnd, me],
                send_sem=sends, recv_sem=recvs.at[rnd % 2],
                device_id=member(d), device_id_type=MESH,
            ).start()

    def every(rnd):
        return pltpu.make_async_remote_copy(
            src_ref=slots.at[rnd, 0 : devices - 1], dst_ref=slots.at[rnd, 0 : devices - 1],
            send_sem=sends, recv_sem=recvs.at[rnd % 2],
            device_id=member(1), device_id_type=MESH,
        )

    def finish_sum(rnd):
        every(rnd).wait_recv()
        every(rnd).wait_send()
        total, rest = exact_tree([slots[rnd, slot] for slot in range(devices)])
        return total / cells, rest / cells

    shape = (padded_count, 128)
    lane = lax.broadcasted_iota(jnp.int32, shape, 1)
    sub = lax.broadcasted_iota(jnp.int32, shape, 0)
    eye = lane == sub
    eye_high = lane == sub + 64
    lane8 = lax.broadcasted_iota(jnp.int32, (8, 128), 1)
    sub8 = lax.broadcasted_iota(jnp.int32, (8, 128), 0)

    def lane_sum(values):
        return jnp.broadcast_to(jnp.sum(values, axis=1, keepdims=True), values.shape)

    def to_column(row, where=eye):
        return lane_sum(jnp.where(where, jnp.broadcast_to(row, shape), 0.0))

    def to_row(column, where=eye):
        return jnp.sum(jnp.where(where, column, 0.0), axis=0, keepdims=True)

    def project(read, count, kind, spans, fresh, square=False):
        every_one = count + square
        for first in range(0, every_one, 20):
            group = range(first, min(first + 20, every_one))

            def step(r, sums):
                at = pl.ds(pl.multiple_of(r * 8, 8), 8)
                other = read(at)
                return tuple(
                    acc + fold_lanes((vecs[i, at, :] if i < count else other) * other)
                    for i, acc in zip(group, sums)
                )

            if fresh:
                sums = (jnp.zeros((8, 128), jnp.float32),) * len(group)
            else:
                sums = tuple(proj[kind, i] for i in group)
            for start, length in spans:
                base = start // 8
                sums = lax.fori_loop(0, length // 8, lambda r, s: step(base + r, s), sums, unroll=4)
            for i, acc in zip(group, sums):
                proj[kind, i] = acc

    def project_late(step, count, p, halo, factor, h):
        square = step == STEPS - 1
        every_one = count + square
        for first in range(0, every_one, 20):
            group = range(first, min(first + 20, every_one))

            def add(r, sums):
                at = pl.ds(pl.multiple_of(p * rows_y + h * rows_half + r * 8, 8), 8)
                other = padded[step, halo, pl.ds(pl.multiple_of(8 + h * rows_half + r * 8, 8), 8), :] * factor
                whole = other
                if every_one in (group.stop,):
                    whole = image[at, :] + other
                    image[at, :] = whole
                return tuple(
                    acc + fold_lanes(vecs[i, at, :] * other if i < count else whole * whole)
                    for i, acc in zip(group, sums)
                )

            sums = lax.fori_loop(0, rows_half // 8, add, tuple(proj[0, i] for i in group), unroll=True)
            for i, acc in zip(group, sums):
                proj[0, i] = acc

    def projected(kind):
        return lane_sum(jnp.sum(proj[kind], axis=1))

    def stencil(step, part, whole=False):
        tall = 16
        lanes = lax.broadcasted_iota(jnp.int32, (tall, width), 1)
        sx, sy, sz = WIND_SPEEDS
        centre = 6.0 + 1.5 * (sx + sy + sz)

        def piece(p, q):
            base = pl.multiple_of(q * tall, 8)
            at = pl.ds(pl.multiple_of(base + 8, 8), tall)
            block = padded[step, p + 2, pl.ds(base, tall + 16), :]
            here = block[8 : tall + 8]
            out_at = pl.ds(pl.multiple_of(p * rows_y + base, 8), tall)
            total = -(react[out_at, :] + centre) * here
            total = total + padded[step, p + 3, at, :] if whole or p < planes - 1 else total
            total = total + (1.0 + 2.0 * sx) * padded[step, p + 1, at, :]
            total = total - (0.5 * sx) * padded[step, p, at, :] if whole or p > 0 else total
            total = total + roll(block, tall + 15, 0)[8 : tall + 8]
            total = total + (1.0 + 2.0 * sy) * roll(block, 1, 0)[8 : tall + 8]
            total = total - (0.5 * sy) * roll(block, 2, 0)[8 : tall + 8]
            total = total + jnp.where(lanes < width - 1, roll(here, width - 1, 1), 0.0)
            total = total + (1.0 + 2.0 * sz) * jnp.where(lanes >= 1, roll(here, 1, 1), 0.0)
            total = total - (0.5 * sz) * jnp.where(lanes >= 2, roll(here, 2, 1), 0.0)
            image[out_at, :] = total

        for p in part:
            @pl.loop(0, rows_y // tall, unroll=True)
            def _(q, p=p):
                piece(p, q)

    def widen(values):
        return jnp.concatenate([values] * (width // 128), axis=1)

    def combine(step, count, scale, inverse=None):
        scale_row = widen(scale)
        more = step < STEPS - 1

        def plane(p, start, tall):
            at = pl.ds(pl.multiple_of(p * rows_y + start, 8), tall)
            total = image[at, :] * scale_row
            for i in range(count):
                total = total - coef[i : i + 1, :] * vecs[i, at, :]
            if more:
                vecs[keep + step, at, :] = total
                padded[step + 1, p + 2, start + 8 : start + 8 + tall, :] = total
            else:
                w_out[step, at, :] = total * widen(inverse)
                if step > 0:
                    w_out[step - 1, at, :] = vecs[keep + step - 1, at, :] * scale_row

        for n, (p_even, p_odd, n_even, n_odd) in enumerate((
            (0, planes - 1, 4, 0),
            (planes - 1, planes - 2, 0, 2),
            (planes - 2, 0, 2, 4),
        )):
            p = jnp.where(even, p_even, p_odd)
            if n > 0:
                plane(p, 0, rows_y)
            for h in range(2):
                if n == 0:
                    plane(p, h * rows_half, rows_half)
                if more:
                    start_halo(step + 1, (n_even + h,), even)
                    start_halo(step + 1, (n_odd + h,), odd)
        for p in range(1, planes - 2):
            plane(p, 0, rows_y)
        if more:
            start_halo(step + 1, (6, 7))

    def outer(a, b):
        return lax.dot_general(
            a, b, (((1,), (1,)), ((), ())), preferred_element_type=jnp.float32
        )

    cut = head.shape[1]
    late = keep * 8 - 128

    def gram_block(r):
        at = pl.ds(pl.multiple_of(r, 8), 8)
        values = vecs[0:keep, at, :].reshape(keep * 8, width)
        power = values * values
        squares[...] = squares[...] + power[:, :128] + power[:, 128:]
        high = values.astype(jnp.bfloat16)
        low = (values - high.astype(jnp.float32)).astype(jnp.bfloat16)
        left = jnp.concatenate([high[:cut] * 0.5, high[cut:]], axis=0)
        first = outer(left, high[:cut]) + outer(low, high[:cut])
        second = outer(low, high[late:])
        third = outer(high[cut:] * 0.5, high[late:])
        return first, second, third

    @pl.loop(0, chunks)
    def _(c):
        @pl.when(c == 1)
        def _():
            pl.semaphore_wait(barrier, expected)
            for d in range(1, n2):
                pl.semaphore_signal(ready, inc=1, device_id=member2(d)[1], device_id_type=MESH)
            pltpu.make_async_copy(all_last, all_last, last_sem).wait()
            start_halo(0, (4, 5, 0, 1, 2, 3), even)
            start_halo(0, (0, 1, 2, 3, 4, 5), odd)
            start_halo(0, (6, 7))

        load(c).wait()
        found = [gram_block(c * CHUNK + s) for s in range(0, CHUNK, 8)]
        first, second, third = (functools.reduce(lambda a, b: a + b, f) for f in zip(*found))
        head[...] = head[...] + first
        tail[...] = tail[...] + second
        tail[cut:, :] = tail[cut:, :] + third

    def picked(values, start):
        row = lax.broadcasted_iota(jnp.int32, values.shape, 0)
        column = lax.broadcasted_iota(jnp.int32, values.shape, 1)
        use = (lax.rem(row, 8) == lax.rem(column, 8)) & (column + start >= (cut if start else 0))
        kept = jnp.where(use, values, 0.0)
        return jnp.sum(kept.reshape(keep, 8, values.shape[1]), axis=1)

    spread = jnp.concatenate([picked(head[...], 0), picked(tail[...], late)], axis=1)
    place = lax.broadcasted_iota(jnp.int32, (cut + 128, 128), 0)
    place = jnp.where(place < cut, place, place - cut + late) // 8
    choose = jnp.where(place == lax.broadcasted_iota(jnp.int32, place.shape, 1), 1.0, 0.0)
    choose = choose.astype(jnp.bfloat16)
    half = jnp.zeros((keep, 128), jnp.float32)
    for _ in range(3):
        term = spread.astype(jnp.bfloat16)
        spread = spread - term.astype(jnp.float32)
        half = half + jnp.dot(term, choose, preferred_element_type=jnp.float32)
    diagonal = jnp.sum(jnp.sum(squares[...].reshape(keep, 8, 128), axis=1), axis=1, keepdims=True)
    lane_k = lax.broadcasted_iota(jnp.int32, (keep, 128), 1)
    sub_k = lax.broadcasted_iota(jnp.int32, (keep, 128), 0)
    pack[...] = jnp.zeros(pack.shape, jnp.float32)
    pack[0:keep] = half
    turned = jnp.transpose(pack[...])
    pack[0:keep] = jnp.where(lane_k == sub_k, diagonal, half + turned[0:keep])
    blocks, start = [], 0
    for b in range(0, keep, 8):
        blocks.append((b, start))
        start += keep - b
    folded = jnp.zeros((8, 128), jnp.float32)
    for b, start in blocks:
        part = jnp.where((lane8 >= b) & (lane8 < keep), pack[b : b + 8], 0.0)
        folded = folded + (roll(part, start - b, 1) if start > b else part)
    grams[me] = folded
    pl.semaphore_wait(ready, n2 - 1)
    for d in range(devices - 1, 0, -1):
        gram_copy(me, d).start()

    def finish_gram():
        arrived = gram_copy(pl.ds(0, devices - 1), 1)
        arrived.wait_recv()
        arrived.wait_send()
        total, rest = exact_tree([grams[slot] for slot in range(devices)])
        ones = jnp.zeros((8, 128), jnp.float32)
        for b, start in blocks:
            ones = jnp.where((lane8 == sub8 + start) & (sub8 + b < keep), cells, ones)
        values = ((ones - total) - rest) / cells
        parts = []
        for b, start in blocks:
            part = roll(values, 128 + b - start, 1) if start > b else values
            parts.append(jnp.where((lane8 >= b) & (lane8 < keep), part, 0.0))
        upper = jnp.concatenate(parts, axis=0)
        pack[0 : 8 * len(parts)] = upper
        lower = jnp.transpose(pack[...])[0 : 8 * len(parts)]
        rows_of = lax.broadcasted_iota(jnp.int32, upper.shape, 0) // 8
        lanes_of = lax.broadcasted_iota(jnp.int32, upper.shape, 1) // 8
        return upper + jnp.where(rows_of > lanes_of, lower, 0.0)

    react_copy.wait()

    everything = [(0, rows)]

    def span(p, n=1):
        return [(p * rows_y, n * rows_y)]

    def project_image(step, spans, fresh=False, square=False):
        project(lambda at: image[at, :], keep + step, 0, spans, fresh, square)

    sx = WIND_SPEEDS[0]
    order = (
        [(0, 0, -0.5 * sx, h, 2 + h) for h in range(2)],
        [(planes - 1, planes + 2, 1.0, h, 4 + h) for h in range(2)],
    )

    def emit(step, scale):
        scale_row = widen(scale)

        @pl.loop(0, rows // 32)
        def _(q):
            at = pl.ds(pl.multiple_of(q * 32, 32), 32)
            w_out[step, at, :] = vecs[keep + step, at, :] * scale_row

    def edges_last(step, count, square, scale):
        wait_halo(step, (6, 7))
        stencil(step, range(2, planes))
        project_image(step, span(2, planes - 3), True, square)
        project_image(step, span(planes - 1))
        if step > 1:
            emit(step - 2, scale)
        wait_halo(step, (0, 1))
        stencil(step, range(2))
        project_image(step, span(0))
        project_image(step, span(1), False, square)
        for first, second in zip(order[0] + order[1], order[1] + order[0]):
            wait_halo(step, (first[4],), even)
            wait_halo(step, (second[4],), odd)
            p, halo, factor = (jnp.where(even, a, b) for a, b in zip(first[:3], second[:3]))
            project_late(step, count, p, halo, factor, first[3])

    gap = None
    scales = jnp.ones(shape, jnp.float32)
    scales_row = jnp.ones((1, 128), jnp.float32)
    lane1 = lax.broadcasted_iota(jnp.int32, (1, 128), 1)
    hess = jnp.zeros((8, 128), jnp.float32)
    b_row = jnp.zeros((1, 128), jnp.float32)
    scale = jnp.ones((1, 128), jnp.float32)
    inverse = None
    for step in range(STEPS):
        count = keep + step
        last = count - 1
        if step > 0:
            project(lambda at: vecs[last, at, :], count, 1, everything, True)
            b_row = to_row(projected(1), eye_high)
        square = step == STEPS - 1
        if step == 0:
            wait_halo(step, range(8))
            stencil(step, range(planes), True)
            project_image(step, everything, True)
        else:
            edges_last(step, count, square, scale)
        row = to_row(projected(0)) + b_row
        begin_sum(step, row)
        drain_halo(step)
        if step == 0:
            gap = finish_gram()
            total, rest = finish_sum(0)
        else:
            total, rest = finish_sum(step)
            overlap = to_column(total, eye_high)
            length = overlap[last : last + 1]
            length_rest = lane_sum(jnp.where(lane1 == 64 + last, rest, 0.0))
            norm = jnp.sqrt(length + EPSILON)
            scale = 1.0 / norm
            hess = jnp.where((sub8 == step - 1) & (lane8 == last), norm, hess)
            scales = jnp.where(sub == last, scale, scales)
            scales_row = jnp.where(lane1 == last, scale, scales_row)
            square, square_rest = two_product(scale, scale)
            unit, unit_rest = two_product(length, square)
            own = (((1.0 - unit) - unit_rest) - length * square_rest) - length_rest * square
            column = jnp.where(sub < last, -overlap * scales * scale, 0.0)
            column = jnp.where(sub == last, own, column)
            gap = jnp.where(sub == last, to_row(column), gap)
            gap = jnp.where(lane == last, column, gap)
        first = jnp.where(sub < count, to_column(total) * scales * scale, 0.0)
        second = lane_sum(gap * to_row(first))
        weights = jnp.where(sub < count, first + second, 0.0)
        scaled = weights * scales
        coef[...] = widen(scaled)
        if step == STEPS - 1:
            parts, parts_rest = two_product(total, scales_row)
            parts_rest = parts_rest + rest * scales_row
            power, power_rest = two_product(parts, parts)
            power_rest = power_rest + 2.0 * parts * parts_rest
            whole = jnp.where(lane1 == count, total, 0.0)
            power = jnp.where(lane1 < count, power, -whole)
            power_rest = jnp.where(lane1 < count, power_rest, jnp.where(lane1 == count, -rest, 0.0))
            grid = lane_sum(whole) * 128.0
            coarse = (power + grid) - grid
            left = -(lane_sum(coarse) + lane_sum((power - coarse) + power_rest))
            third = lane_sum(gap * to_row(second))
            left = left * scale * scale - jnp.sum(first * second + weights * third, axis=0, keepdims=True)
            norm = jnp.sqrt(jnp.maximum(left, 0.0) + EPSILON)
            inverse = 1.0 / norm
            hess = jnp.where((sub8 == step) & (lane8 == count), norm, hess)
        hess = jnp.where((sub8 == step) & (lane8 < count), to_row(weights), hess)
        if step == STEPS - 1:
            h_out[...] = hess
        combine(step, count, scale, inverse)


def group_of(count):
    for size in (4, 2):
        if count % size == 0:
            return size
    return 1


def body(basis_vectors, reaction):
    keep, planes, rows_y, width = basis_vectors.shape
    n_gx, n_gy = lax.axis_size("gx"), lax.axis_size("gy")
    g1 = group_of(n_gx)
    size = keep + STEPS
    padded_count = -(-size // 8) * 8
    rows = planes * rows_y
    rounds = STEPS
    f32 = jnp.float32
    dma = pltpu.SemaphoreType.DMA
    held = [
        pltpu.with_memory_space_constraint(x, pltpu.HBM)
        for x in (basis_vectors.reshape(keep, rows, width), reaction.reshape(rows, width))
    ]
    w, h = pl.pallas_call(
        functools.partial(kernel, keep, planes, rows_y, n_gx, n_gy, g1),
        out_shape=(
            jax.ShapeDtypeStruct((STEPS, rows, width), f32),
            jax.ShapeDtypeStruct((8, 128), f32),
        ),
        in_specs=[pl.BlockSpec(memory_space=pltpu.HBM)] * 2,
        out_specs=(pl.BlockSpec(memory_space=pltpu.VMEM),) * 2,
        scratch_shapes=[
            pltpu.VMEM((size, rows, width), f32),
            pltpu.VMEM((STEPS, planes + 3, rows_y + 16, width), f32),
            pltpu.VMEM((rows, width), f32),
            pltpu.VMEM((rows, width), f32),
            pltpu.VMEM((keep * 8, 256), f32),
            pltpu.VMEM((keep * 8, 128), f32),
            pltpu.VMEM((keep * 8, 128), f32),
            pltpu.VMEM((128, 128), f32),
            pltpu.VMEM((2, padded_count, 8, 128), f32),
            pltpu.VMEM((n_gx * n_gy, 8, 128), f32),
            pltpu.VMEM((rounds, n_gx * n_gy, 1, 128), f32),
            pltpu.VMEM((padded_count, width), f32),
            dma((rows // CHUNK,)),
            dma,
            dma,
            dma((4,)),
            dma((8,)),
            dma,
            dma,
            dma,
            dma((2,)),
            pltpu.SemaphoreType.REGULAR,
        ],
        compiler_params=pltpu.CompilerParams(
            collective_id=0, has_side_effects=True, vmem_limit_bytes=48 * 1024 * 1024
        ),
    )(*held)
    return w.reshape(STEPS, planes, rows_y, width), h[:STEPS, :size].T


def solution(mesh):
    in_specs = (P(None, "gx", "gy", None), P("gx", "gy", None))
    out_specs = (P(None, "gx", "gy", None), P())
    return jax.shard_map(body, mesh=mesh, in_specs=in_specs, out_specs=out_specs, check_vma=False)
```
